512 devices in a mesh: blk: 16 (over x, y_hi, core), vox: 32 (over z, y_lo).
Axes of the slice: x: 4, y: 4 (y_hi: 2, y_lo: 2; y = y_hi * 2 + y_lo), z: 16, core: 2. Of those that a mesh axis runs over, the one named last changes fastest.
Arguments:
- src_fields: bfloat16 [1024, 131072], P('blk', 'vox'), may hold values from -6 to 6
- det_fields: bfloat16 [1024, 131072], P('blk', 'vox'), may hold values from -6 to 6
- probes: bfloat16 [2, 131072], P(None, 'vox'), may hold values from -6 to 6
Outputs:
- curvature: float32 [2, 131072], P(None, 'vox')
The draws below stay inside these ranges and needn't reach their ends.
All inputs are finite; a program needn't handle non-finite values.
Results may differ from the reference program's by a relative error of at most 0.0016.
Values may be sent and summed in bfloat16 or wider, within the bound.
A program may use at most 64 MiB of HBM per device.

```python
import jax
import jax.numpy as jnp
from jax import lax

PROBES = 2
VOX_DEV = 4096
SOURCES = 1024
DETECTORS = 1024
VOXELS = 131072
N_VOX = 32


def levels(stream_key, extent, split, low, top_value):
    def one(position, shards_of):
        heights = jax.random.uniform(jax.random.fold_in(jax.random.fold_in(stream_key, 6), position), (shards_of,), jnp.float32, low / len(split), top_value / len(split))
        return jnp.repeat(jnp.exp(heights), extent[position] // shards_of).reshape((-1,) + (1,) * (len(extent) - position - 1))

    gain = one(*split[0])
    for cut in split[1:]:
        gain = gain * one(*cut)
    return gain


def bell_draw(own_key, shape, scale, bound, shards=(), kind=jnp.bfloat16):
    values = jax.random.normal(own_key, shape, jnp.float32) * scale
    if len(shards) > 0:
        values = levels(own_key, shape, shards, -0.22, 0.18) * values
    return jnp.clip(values, min=-bound, max=bound).astype(kind)


def setup_inputs(seed: int = 0) -> dict:
    keys = jax.random.split(jax.random.key(seed), 4)
    src_fields = bell_draw(keys[0], (SOURCES, VOXELS), 1.0, 6.0, ((0, 16), (1, 32)))
    det_fields = bell_draw(keys[1], (DETECTORS, VOXELS), 1.0, 6.0, ((0, 16), (1, 32)))
    probes = bell_draw(keys[2], (PROBES, VOXELS), 1.0, 6.0, ((1, 32),))
    return {"src_fields": src_fields, "det_fields": det_fields, "probes": probes}


def reference(src_fields, det_fields, probes):
    def measure(probe_row):
        weighted = (src_fields.astype(jnp.float32) * probe_row.astype(jnp.float32)[None, :]).astype(jnp.bfloat16)
        return jnp.dot(weighted, det_fields.T, preferred_element_type=jnp.float32)

    measured = lax.map(measure, probes)
    measured_b = measured.astype(jnp.bfloat16).astype(jnp.float32)
    src_blocks = src_fields.reshape(SOURCES, N_VOX, VOX_DEV).transpose(1, 0, 2)
    det_blocks = det_fields.reshape(DETECTORS, N_VOX, VOX_DEV).transpose(1, 0, 2)

    def adjoint(pair):
        src_block, det_block = pair
        backproj = jnp.einsum("ksd,dv->ksv", measured_b, det_block.astype(jnp.float32), precision=lax.Precision.HIGHEST)
        return jnp.sum(src_block.astype(jnp.float32)[None] * backproj, axis=1)

    blocks = lax.map(adjoint, (src_blocks, det_blocks))
    total = blocks.transpose(1, 0, 2).reshape(PROBES, VOXELS)
    return total / jnp.float32(SOURCES * DETECTORS)
```

```python
import functools

import jax
import jax.numpy as jnp
from jax import lax
from jax.experimental import pallas as pl
from jax.experimental.pallas import tpu as pltpu
from jax.sharding import PartitionSpec as P

MESH = pl.DeviceIdType.MESH
BF16 = jnp.bfloat16
F32 = jnp.float32
DMA = pltpu.SemaphoreType.DMA

NX, NY, NZ, NC = 4, 4, 16, 2
NQ = 8


def device(x, y, z, c):
    return (x * 4 + (y // 2) * 2 + c, z * 2 + y % 2)


def send(src, dst, send_sem, recv_sem, to):
    pltpu.make_async_remote_copy(
        src_ref=src, dst_ref=dst, send_sem=send_sem, recv_sem=recv_sem, device_id=to, device_id_type=MESH
    ).start()


def wait_for(ref, sem):
    pltpu.make_async_copy(ref, ref, sem).wait()


def kernel(
    scale,
    src_hbm,
    det_hbm,
    probes_hbm,
    out,
    src_v,
    det_v,
    pr_v,
    pr_in,
    pr_f,
    S,
    D,
    acc,
    tx1P,
    tx1Q,
    rx1P,
    rx1Q,
    tx2P,
    tx2Q,
    rx2P,
    rx2Q,
    zs,
    zr,
    mz,
    MP,
    MQ,
    cv,
    cr,
    fin,
    ob,
    ld,
    ysend,
    yS,
    yD,
    xsend,
    xS,
    xD,
    c0,
    c1,
    r1send,
    r1P,
    r1Q,
    r2send,
    r2P,
    r2Q,
    zsend,
    zrecv,
    gsend,
    grecv,
    asend,
    aP,
    aQ,
    bsend,
    bP,
    bQ,
    csend,
    crecv,
    fsend,
    frecv,
):
    blk = lax.axis_index("blk")
    vox = lax.axis_index("vox")
    x, yh, c = blk // 4, (blk // 2) % 2, blk % 2
    z, yl = vox // 2, vox % 2
    y = yh * 2 + yl
    half = src_v.shape[1] // 2
    vc = half // NQ

    up, down = (y + 1) % NY, (y + 3) % NY
    u, v = (yh + yl) % 2, yh
    ya, yb = yh * 2 + 1 - yl, 3 - y
    xs = (x // 2) * 2 + 1 - x % 2
    xd = 3 - x
    zg, zt = z // 4, z % 4

    dev_up, dev_down = device(x, up, z, c), device(x, down, z, c)
    dev_a, dev_b = device(x, ya, z, c), device(x, yb, z, c)
    dev_xs, dev_xd = device(xs, y, z, c), device(xd, y, z, c)
    dev_c = device(x, y, z, 1 - c)
    me = x * 2 + c

    pltpu.make_async_copy(det_hbm, det_v, ld.at[0]).start()
    pltpu.make_async_copy(src_hbm, src_v, ld.at[1]).start()
    pltpu.make_async_copy(probes_hbm, pr_v, ld.at[2]).start()

    barrier = pltpu.get_barrier_semaphore()

    def greet_z(j, carry):
        pl.semaphore_signal(barrier, inc=1, device_id=device(x, y, (z + j) % NZ, c), device_id_type=MESH)
        return carry

    lax.fori_loop(1, NZ, greet_z, 0)

    def greet_plane(j, carry):
        e = (me + j) % NQ
        pl.semaphore_signal(barrier, inc=1, device_id=device(e // 2, y, z, e % 2), device_id_type=MESH)
        return carry

    lax.fori_loop(1, NQ, greet_plane, 0)

    def greet_rows(e, carry):
        pl.semaphore_signal(barrier, inc=1, device_id=device(e // 2, up, z, e % 2), device_id_type=MESH)
        pl.semaphore_signal(barrier, inc=1, device_id=device(e // 2, down, z, e % 2), device_id_type=MESH)
        return carry

    lax.fori_loop(0, NQ, greet_rows, 0)
    pl.semaphore_wait(barrier, NZ - 1 + NQ - 1 + 2 * NQ)

    h_up, h_down = up // 2, down // 2
    mine = pl.ds(pl.multiple_of(yh * 64, 64), 64)
    wait_for(det_v, ld.at[0])
    wait_for(src_v, ld.at[1])
    wait_for(pr_v, ld.at[2])
    send(
        pr_v.at[:, pl.ds(pl.multiple_of(h_up * half, half), half)],
        pr_in,
        ysend.at[2],
        ysend.at[3],
        dev_up,
    )

    def spread(q, carry):
        to_up = pl.ds(pl.multiple_of(h_up * half + q * vc, vc), vc)
        to_down = pl.ds(pl.multiple_of(h_down * half + q * vc, vc), vc)
        send(det_v.at[:, to_up], D.at[q, mine], ysend.at[0], yD.at[q], dev_up)
        send(det_v.at[:, to_down], D.at[q, mine], ysend.at[0], yD.at[q], dev_down)
        send(src_v.at[:, to_up], S.at[q, mine], ysend.at[1], yS.at[q], dev_up)
        send(src_v.at[:, to_down], S.at[q, mine], ysend.at[1], yS.at[q], dev_down)
        return carry

    lax.fori_loop(0, NQ, spread, 0)

    acc[...] = jnp.zeros_like(acc)
    wait_for(pr_in, ysend.at[3])
    for q in range(NQ):
        pr_f[q] = pr_in[:, q * vc : (q + 1) * vc].astype(F32)

    own, other = pl.ds(0, 128), pl.ds(128, 128)

    def pass_own(q):
        wait_for(D.at[q, own], yD.at[q])
        send(D.at[q, own], D.at[q, other], xsend.at[1], xD.at[q], dev_xd)
        send(D.at[q, own], D.at[q, pl.ds(256, 128)], xsend.at[2], c0.at[q], dev_c)
        wait_for(S.at[q, own], yS.at[q])
        send(S.at[q, own], S.at[q, other], xsend.at[0], xS.at[q], dev_xs)

    def pass_other(q):
        wait_for(D.at[q, other], xD.at[q])
        send(D.at[q, other], D.at[q, pl.ds(384, 128)], xsend.at[3], c1.at[q], dev_c)

    def measure(q):
        wait_for(S.at[q, other], xS.at[q])
        wait_for(D.at[q, pl.ds(256, 128)], c0.at[q])
        wait_for(D.at[q, pl.ds(384, 128)], c1.at[q])
        fields = S[q].astype(F32)
        p = pr_f[q]
        det = D[q]
        for k in range(2):
            weighted = (fields * p[k : k + 1]).astype(BF16)
            part = lax.dot_general(weighted, det, (((1,), (1,)), ((), ())), preferred_element_type=F32)
            for g in range(4):
                acc[g, k] += part[:, g * 128 : (g + 1) * 128].reshape(2, 2, 64, 128)

    pass_own(0)
    pass_own(1)
    pass_other(0)

    def gather(q, carry):
        pass_own(q)
        pass_other(q - 1)
        measure(q - 2)
        return carry

    lax.fori_loop(2, NQ, gather, 0)
    pass_other(NQ - 1)
    measure(NQ - 2)
    measure(NQ - 1)

    groups = [(zg + o) % 4 for o in (2, 1, 3, 0)]
    for i, g in enumerate(groups):
        tx1P[i] = acc[g, 0, 1 - u].astype(BF16)
        send(tx1P.at[i], rx1P.at[i], r1send.at[0], r1P.at[i], dev_a)
        tx1Q[i, 0] = acc[g, 1, 0, 1 - v].astype(BF16)
        tx1Q[i, 1] = acc[g, 1, 1, 1 - v].astype(BF16)
        send(tx1Q.at[i], rx1Q.at[i], r1send.at[1], r1Q.at[i], dev_b)

    def second(i):
        g = groups[i]
        wait_for(rx1P.at[i], r1P.at[i])
        tx2P[i] = (acc[g, 0, u, 1 - v] + rx1P[i, 1 - v].astype(F32)).astype(BF16)
        send(tx2P.at[i], rx2P.at[i], r2send.at[0], r2P.at[i], dev_b)
        wait_for(rx1Q.at[i], r1Q.at[i])
        tx2Q[i] = (acc[g, 1, 1 - u, v] + rx1Q[i, 1 - u].astype(F32)).astype(BF16)
        send(tx2Q.at[i], rx2Q.at[i], r2send.at[1], r2Q.at[i], dev_a)
        acc[g, 0, u, v] += rx1P[i, v].astype(F32)
        acc[g, 1, u, v] += rx1Q[i, u].astype(F32)

    def third(i):
        g = groups[i]
        wait_for(rx2P.at[i], r2P.at[i])
        zs[i, :, 0] = (acc[g, 0, u, v] + rx2P[i].astype(F32)).reshape(4, 16, 128).astype(BF16)
        wait_for(rx2Q.at[i], r2Q.at[i])
        zs[i, :, 1] = (acc[g, 1, u, v] + rx2Q[i].astype(F32)).reshape(4, 16, 128).astype(BF16)
        for j in range(4):
            t = (zt + 4 - j) % 4
            if i == 3 and j == 0:
                continue
            send(zs.at[i, t], zr.at[z], zsend, zrecv, device(x, y, g * 4 + t, c))

    second(0)
    second(1)
    third(0)
    second(2)
    third(1)
    second(3)
    third(2)
    third(3)
    zr[z] = zs[3, zt]
    wait_for(zr.at[pl.ds(0, NZ - 1)], zrecv)
    total = zr[0].astype(F32)
    for j in range(1, NZ):
        total += zr[j].astype(F32)
    mz[...] = total.astype(BF16)

    MP[zg, u, v, zt] = mz[0]
    MQ[zg, u, v, zt] = mz[1]
    for j in range(NZ - 1):
        step = NZ // 2 + ((j + 1) // 2) * (1 if j % 2 else -1)
        to = device(x, y, (z + step) % NZ, c)
        send(mz.at[0], MP.at[zg, u, v, zt], gsend, grecv.at[zg], to)
        send(mz.at[1], MQ.at[zg, u, v, zt], gsend, grecv.at[zg], to)

    back = [(zg + o) % 4 for o in (0, 1, 3, 2)]

    def first_back(i):
        g = back[i]
        wait_for(zr.at[pl.ds(0, 4 if i else 3)], grecv.at[g])
        send(MP.at[g, u, v], MP.at[g, u, v], asend.at[0], aP.at[g], dev_b)
        send(MQ.at[g, u, v], MQ.at[g, u, v], asend.at[1], aQ.at[g], dev_a)

    def second_back(i):
        g = back[i]
        wait_for(MP.at[g, u, 1 - v], aP.at[g])
        send(MP.at[g, u], MP.at[g, u], bsend.at[0], bP.at[g], dev_a)
        wait_for(MQ.at[g, 1 - u, v], aQ.at[g])
        send(MQ.at[g, 0, v], MQ.at[g, 0, v], bsend.at[1], bQ.at[g], dev_b)
        send(MQ.at[g, 1, v], MQ.at[g, 1, v], bsend.at[1], bQ.at[g], dev_b)

    def third_back(i):
        g = back[i]
        wait_for(MP.at[g, 1 - u], bP.at[g])
        wait_for(MQ.at[g, 1 - u], bQ.at[g])

    def contribution(q, lo):
        g0, g1 = back[lo], back[lo + 1]
        det = jnp.concatenate(
            [
                D[q, pl.ds(pl.multiple_of(g0 * 128, 128), 128)],
                D[q, pl.ds(pl.multiple_of(g1 * 128, 128), 128)],
            ],
            axis=0,
        )
        fields = S[q].astype(F32)
        rows = []
        for m in (MP, MQ):
            lhs = jnp.concatenate([m[g0].reshape(256, 128), m[g1].reshape(256, 128)], axis=1)
            bp = jnp.dot(lhs, det, preferred_element_type=F32)
            rows.append(jnp.sum(fields * bp, axis=0, keepdims=True))
        return jnp.concatenate(rows, axis=0)

    first_back(0)
    first_back(1)
    second_back(0)
    first_back(2)
    second_back(1)
    first_back(3)
    third_back(0)
    third_back(1)

    second_back(2)

    def front(q, carry):
        cv[q] = contribution(q, 0)
        return carry

    lax.fori_loop(0, NQ, front, 0)
    second_back(3)
    third_back(2)
    third_back(3)

    def rest(j, carry):
        q = (me + j) % NQ
        cv[q] = cv[q] + contribution(q, 2)
        send(cv.at[q], cr.at[me], csend, crecv, device(q // 2, y, z, q % 2))
        return carry

    lax.fori_loop(1, NQ, rest, 0)
    cr[me] = cv[me] + contribution(me, 2)
    wait_for(cr.at[pl.ds(0, NQ - 1)], crecv)
    whole = cr[0]
    for j in range(1, NQ):
        whole += cr[j]
    fin[...] = whole * scale

    def hand_out(e, carry):
        send(fin, ob.at[yh, me], fsend, frecv, device(e // 2, up, z, e % 2))
        send(fin, ob.at[yh, me], fsend, frecv, device(e // 2, down, z, e % 2))
        return carry

    lax.fori_loop(0, NQ, hand_out, 0)

    wait_for(det_v, ysend.at[0])
    wait_for(src_v, ysend.at[1])
    wait_for(pr_in, ysend.at[2])
    wait_for(S.at[:, own], xsend.at[0])
    wait_for(D.at[:, own], xsend.at[1])
    wait_for(D.at[:, own], xsend.at[2])
    wait_for(D.at[:, own], xsend.at[3])
    wait_for(tx1P, r1send.at[0])
    wait_for(tx1Q, r1send.at[1])
    wait_for(tx2P, r2send.at[0])
    wait_for(tx2Q, r2send.at[1])
    wait_for(zr.at[pl.ds(0, NZ - 1)], zsend)
    wait_for(zr.at[pl.ds(0, NZ - 1)], gsend)
    wait_for(tx2P, asend.at[0])
    wait_for(tx2P, asend.at[1])
    wait_for(tx1P, bsend.at[0])
    wait_for(tx1P, bsend.at[1])
    wait_for(cr.at[pl.ds(0, NQ - 1)], csend)
    wait_for(ob, frecv)
    for h in range(2):
        for e in range(NQ):
            at = h * half + e * vc
            out[:, at : at + vc] = ob[h, e]
    wait_for(ob, fsend)


def shards(src_fields, det_fields, probes):
    rows, voxels = src_fields.shape
    half = voxels // 2
    vc = half // NQ
    sources, detectors = rows * lax.axis_size("blk"), det_fields.shape[0] * lax.axis_size("blk")
    scale = 1.0 / (sources * detectors)
    any_spec = pl.BlockSpec(memory_space=pl.ANY)
    return pl.pallas_call(
        functools.partial(kernel, scale),
        out_shape=jax.ShapeDtypeStruct((2, voxels), F32),
        in_specs=[any_spec] * 3,
        out_specs=pl.BlockSpec(memory_space=pltpu.VMEM),
        scratch_shapes=[
            pltpu.VMEM((64, voxels), BF16),
            pltpu.VMEM((64, voxels), BF16),
            pltpu.VMEM((2, voxels), BF16),
            pltpu.VMEM((2, half), BF16),
            pltpu.VMEM((NQ, 2, vc), F32),
            pltpu.VMEM((NQ, 256, vc), BF16),
            pltpu.VMEM((NQ, 512, vc), BF16),
            pltpu.VMEM((4, 2, 2, 2, 64, 128), F32),
            pltpu.VMEM((4, 2, 64, 128), BF16),
            pltpu.VMEM((4, 2, 64, 128), BF16),
            pltpu.VMEM((4, 2, 64, 128), BF16),
            pltpu.VMEM((4, 2, 64, 128), BF16),
            pltpu.VMEM((4, 64, 128), BF16),
            pltpu.VMEM((4, 64, 128), BF16),
            pltpu.VMEM((4, 64, 128), BF16),
            pltpu.VMEM((4, 64, 128), BF16),
            pltpu.VMEM((4, 4, 2, 16, 128), BF16),
            pltpu.VMEM((NZ, 2, 16, 128), BF16),
            pltpu.VMEM((2, 16, 128), BF16),
            pltpu.VMEM((4, 2, 2, 4, 16, 128), BF16),
            pltpu.VMEM((4, 2, 2, 4, 16, 128), BF16),
            pltpu.VMEM((NQ, 2, vc), F32),
            pltpu.VMEM((NQ, 2, vc), F32),
            pltpu.VMEM((2, vc), F32),
            pltpu.VMEM((2, NQ, 2, vc), F32),
            DMA((3,)),
            DMA((4,)),
            DMA((NQ,)),
            DMA((NQ,)),
            DMA((4,)),
            DMA((NQ,)),
            DMA((NQ,)),
            DMA((NQ,)),
            DMA((NQ,)),
            DMA((2,)),
            DMA((4,)),
            DMA((4,)),
            DMA((2,)),
            DMA((4,)),
            DMA((4,)),
            DMA,
            DMA,
            DMA,
            DMA((4,)),
            DMA((2,)),
            DMA((4,)),
            DMA((4,)),
            DMA((2,)),
            DMA((4,)),
            DMA((4,)),
            DMA,
            DMA,
            DMA,
            DMA,
        ],
        compiler_params=pltpu.CompilerParams(collective_id=0, has_side_effects=True),
        name="gauss_newton",
    )(src_fields, det_fields, probes)


def solution(mesh):
    return jax.shard_map(
        shards,
        mesh=mesh,
        in_specs=(P("blk", "vox"), P("blk", "vox"), P(None, "vox")),
        out_specs=P(None, "vox"),
        check_vma=False,
    )
```

```python
import functools

import jax
import jax.numpy as jnp
from jax import lax
from jax.experimental import pallas as pl
from jax.experimental.pallas import tpu as pltpu
from jax.sharding import PartitionSpec as P

MESH = pl.DeviceIdType.MESH
BF16 = jnp.bfloat16
F32 = jnp.float32
DMA = pltpu.SemaphoreType.DMA

NX, NY, NZ, NC = 4, 4, 16, 2
NQ = 8
NB = 4


def device(x, y, z, c):
    return (x * 4 + (y // 2) * 2 + c, z * 2 + y % 2)


def send(src, dst, send_sem, recv_sem, to):
    pltpu.make_async_remote_copy(
        src_ref=src, dst_ref=dst, send_sem=send_sem, recv_sem=recv_sem, device_id=to, device_id_type=MESH
    ).start()


def wait_for(ref, sem):
    pltpu.make_async_copy(ref, ref, sem).wait()


def kernel(
    scale,
    src_hbm,
    det_hbm,
    probes_hbm,
    out,
    src_v,
    det_v,
    pr_v,
    pr_in,
    S,
    D,
    acc,
    tx,
    rx,
    zs,
    zr,
    mz,
    M,
    part,
    cv,
    ob,
    ld,
    ysend,
    yS,
    yD,
    pS,
    xsend,
    xS,
    xD,
    c0,
    c1,
    rsend,
    rrecv,
    zsend,
    zrecv,
    gsend,
    grecv,
    asend,
    arecv,
    fsend,
    frecv,
    ready,
):
    blk = lax.axis_index("blk")
    vox = lax.axis_index("vox")
    x, yh, c = blk // 4, (blk // 2) % 2, blk % 2
    z, yl = vox // 2, vox % 2
    y = yh * 2 + yl
    half = src_v.shape[1] // 2
    vc = half // NQ
    scope = jax.named_scope

    up, down = (y + 1) % NY, (y + 3) % NY
    xs = (x // 2) * 2 + 1 - x % 2
    xd = 3 - x
    zg, zt = z // 4, z % 4
    me = x * 2 + c
    dev_up, dev_down = device(x, up, z, c), device(x, down, z, c)
    dev_xs, dev_xd = device(xs, y, z, c), device(xd, y, z, c)
    dev_c = device(x, y, z, 1 - c)

    def dev_z(d):
        return device(x, y, (z + NZ + d) % NZ, c)

    def signal(sem, to):
        pl.semaphore_signal(sem, inc=1, device_id=to, device_id_type=MESH)

    barrier = pltpu.get_barrier_semaphore()
    near = (dev_up, dev_down, dev_xs, dev_xd, dev_c, dev_z(1), dev_z(-1))
    for to in near:
        signal(barrier, to)

    h_up, h_down = up // 2, down // 2

    def columns(h, q):
        return pl.ds(pl.multiple_of(h * half + q * vc, vc), vc)

    pltpu.make_async_copy(probes_hbm, pr_v, ld.at[NQ]).start()
    for q in range(NQ):
        for h in range(2):
            at = pl.ds(h * half + q * vc, vc)
            pltpu.make_async_copy(det_hbm.at[:, at], det_v.at[:, at], ld.at[q]).start()
            pltpu.make_async_copy(src_hbm.at[:, at], src_v.at[:, at], ld.at[q]).start()
    with scope("t_barrier"):
        pl.semaphore_wait(barrier, len(near))

    def spread_word(r):
        d = 2**r
        if r:
            pl.semaphore_wait(ready.at[r - 1], 2)
        if r < 3:
            signal(ready.at[r], dev_z(d))
            signal(ready.at[r], dev_z(-d))

    mine = pl.ds(pl.multiple_of(yh * 64, 64), 64)
    own, other = pl.ds(0, 128), pl.ds(128, 128)
    for q in range(NQ):
        with scope("t_load%d" % q):
            wait_for(D.at[q, pl.ds(0, 256)], ld.at[q])
        send(det_v.at[:, columns(h_up, q)], D.at[q, mine], ysend.at[0], yD.at[q], dev_up)
        send(det_v.at[:, columns(h_down, q)], D.at[q, mine], ysend.at[0], yD.at[q], dev_down)
        send(src_v.at[:, columns(h_up, q)], S.at[q, mine], ysend.at[1], yS.at[q], dev_up)
        send(src_v.at[:, columns(h_down, q)], S.at[q, mine], ysend.at[1], yS.at[q], dev_down)
        if q == 0:
            wait_for(pr_v, ld.at[NQ])
            send(
                pr_v.at[:, pl.ds(pl.multiple_of(h_up * half, half), half)],
                pr_in,
                ysend.at[2],
                pS,
                dev_up,
            )
            spread_word(0)

    def pass_own(q):
        wait_for(D.at[q, own], yD.at[q])
        send(D.at[q, own], D.at[q, other], xsend.at[1], xD.at[q], dev_xd)
        send(D.at[q, own], D.at[q, pl.ds(256, 128)], xsend.at[2], c0.at[q], dev_c)
        wait_for(S.at[q, own], yS.at[q])
        send(S.at[q, own], S.at[q, other], xsend.at[0], xS.at[q], dev_xs)

    def pass_other(q):
        wait_for(D.at[q, other], xD.at[q])
        send(D.at[q, other], D.at[q, pl.ds(384, 128)], xsend.at[3], c1.at[q], dev_c)

    def measure(q):
        wait_for(S.at[q, other], xS.at[q])
        wait_for(D.at[q, pl.ds(256, 128)], c0.at[q])
        wait_for(D.at[q, pl.ds(384, 128)], c1.at[q])
        fields = S[q].astype(F32)
        p = pr_in[:, q * vc : (q + 1) * vc].astype(F32)
        det = D[q]
        for k in range(2):
            weighted = (fields * p[k : k + 1]).astype(BF16)
            sums = lax.dot_general(weighted, det, (((1,), (1,)), ((), ())), preferred_element_type=F32)
            for g in range(4):
                piece = sums[:, g * 128 : (g + 1) * 128].reshape(4, 64, 128)
                if q:
                    acc[g, :, k] += piece
                else:
                    acc[g, :, k] = piece

    word = {1: 1, 4: 2, 7: 3}
    for t in range(NQ + 4):
        if t < NQ:
            with scope("g%02d_own" % t):
                pass_own(t)
        if t in word:
            with scope("g%02d_word" % t):
                spread_word(word[t])
        if 0 <= t - 3 < NQ:
            with scope("g%02d_other" % t):
                pass_other(t - 3)
        if t == 4:
            wait_for(pr_in, pS)
        if 0 <= t - 4 < NQ:
            with scope("g%02d_meas" % t):
                measure(t - 4)

    groups = [(zg + o) % 4 for o in (2, 1, 3, 0)]
    for i, g in enumerate(groups):
        for d in (2, 1, 3):
            to = (y + d) % NY
            tx[i, to] = acc[g, to].astype(BF16)
            send(tx.at[i, to], rx.at[i, y], rsend, rrecv.at[i], device(x, to, z, c))

    for i, g in enumerate(groups):
        with scope("r%d_y" % i):
            wait_for(rx.at[i, pl.ds(0, 3)], rrecv.at[i])
        total = acc[g, y]
        for d in (1, 2, 3):
            total += rx[i, (y + d) % NY].astype(F32)
        total = total.astype(BF16)
        for k in range(2):
            zs[i, :, k] = total[k].reshape(4, 16, 128)
        for j in range(4):
            t = (zt + 4 - j) % 4
            if i == 3 and j == 0:
                continue
            send(zs.at[i, t], zr.at[z], zsend, zrecv, device(x, y, g * 4 + t, c))
    zr[z] = zs[3, zt]
    with scope("r_z"):
        wait_for(zr.at[pl.ds(0, NZ - 1)], zrecv)
    total = zr[0].astype(F32)
    for j in range(1, NZ):
        total += zr[j].astype(F32)
    mz[...] = total.astype(BF16)

    M[zg, y, zt] = mz[...]
    for j in range(NZ - 1):
        step = NZ // 2 + ((j + 1) // 2) * (1 if j % 2 else -1)
        send(mz, M.at[zg, y, zt], gsend, grecv.at[zg], dev_z(step))

    back = [(zg + o) % 4 for o in (0, 1, 3, 2)]
    for i, g in enumerate(back):
        with scope("b%d_z" % i):
            wait_for(zr.at[pl.ds(0, 4 if i else 3)], grecv.at[g])
        for d in (2, 1, 3):
            send(M.at[g, y], M.at[g, y], asend, arecv.at[g], device(x, (y + d) % NY, z, c))

    def contribution(q, lo):
        lhs = jnp.concatenate([M[back[i]].reshape(512, 128) for i in (lo, lo + 1)], axis=1)
        det = jnp.concatenate(
            [D[q, pl.ds(pl.multiple_of(back[i] * 128, 128), 128)] for i in (lo, lo + 1)], axis=0
        )
        bp = jnp.dot(lhs, det, preferred_element_type=F32).reshape(16, 2, 16, vc)
        fields = S[q].astype(F32).reshape(16, 16, vc)
        rows = [jnp.sum(jnp.sum(fields * bp[:, k], axis=0), axis=0, keepdims=True) for k in range(2)]
        return jnp.concatenate(rows, axis=0)

    for i in range(2):
        with scope("b%d_y" % i):
            wait_for(M.at[back[i], pl.ds(0, 3)], arecv.at[back[i]])
    with scope("m_front"):
        for q in range(NQ):
            part[q] = contribution(q, 0)
    for i in range(2, 4):
        with scope("b%d_y" % i):
            wait_for(M.at[back[i], pl.ds(0, 3)], arecv.at[back[i]])

    per = NQ // NB
    with scope("m_rest"):
        for b in range(NB):
            for a in range(per):
                q = b * per + a
                cv[b, :, a * vc : (a + 1) * vc] = part[q] + contribution(q, 2)
            for e in range(NX * NC):
                for to in (up, down):
                    send(cv.at[b], ob.at[yh, me, b], fsend, frecv, device(e // 2, to, z, e % 2))
    with scope("f_recv"):
        wait_for(ob, frecv)
    wide = half // NB
    for h in range(2):
        for b in range(NB):
            whole = ob[h, 0, b]
            for e in range(1, NX * NC):
                whole += ob[h, e, b]
            at = h * half + b * wide
            out[:, at : at + wide] = whole * scale

    wait_for(det_v, ysend.at[0])
    wait_for(src_v, ysend.at[1])
    wait_for(pr_in, ysend.at[2])
    wait_for(S.at[:, own], xsend.at[0])
    for i in (1, 2, 3):
        wait_for(D.at[:, own], xsend.at[i])
    wait_for(tx.at[:, pl.ds(0, 3)], rsend)
    wait_for(zr.at[pl.ds(0, NZ - 1)], zsend)
    wait_for(zr.at[pl.ds(0, NZ - 1)], gsend)
    wait_for(M.at[:, pl.ds(0, 3)], asend)
    wait_for(ob, fsend)


def shards(src_fields, det_fields, probes):
    rows, voxels = src_fields.shape
    half = voxels // 2
    vc = half // NQ
    sources, detectors = rows * lax.axis_size("blk"), det_fields.shape[0] * lax.axis_size("blk")
    scale = 1.0 / (sources * detectors)
    any_spec = pl.BlockSpec(memory_space=pl.ANY)
    return pl.pallas_call(
        functools.partial(kernel, scale),
        out_shape=jax.ShapeDtypeStruct((2, voxels), F32),
        in_specs=[any_spec] * 3,
        out_specs=pl.BlockSpec(memory_space=pltpu.VMEM),
        scratch_shapes=[
            pltpu.VMEM((64, voxels), BF16),
            pltpu.VMEM((64, voxels), BF16),
            pltpu.VMEM((2, voxels), BF16),
            pltpu.VMEM((2, half), BF16),
            pltpu.VMEM((NQ, 256, vc), BF16),
            pltpu.VMEM((NQ, 512, vc), BF16),
            pltpu.VMEM((4, 4, 2, 64, 128), F32),
            pltpu.VMEM((4, 4, 2, 64, 128), BF16),
            pltpu.VMEM((4, 4, 2, 64, 128), BF16),
            pltpu.VMEM((4, 4, 2, 16, 128), BF16),
            pltpu.VMEM((NZ, 2, 16, 128), BF16),
            pltpu.VMEM((2, 16, 128), BF16),
            pltpu.VMEM((4, 4, 4, 2, 16, 128), BF16),
            pltpu.VMEM((NQ, 2, vc), F32),
            pltpu.VMEM((NB, 2, half // NB), F32),
            pltpu.VMEM((2, NX * NC, NB, 2, half // NB), F32),
            DMA((NQ + 1,)),
            DMA((3,)),
            DMA((NQ,)),
            DMA((NQ,)),
            DMA,
            DMA((4,)),
            DMA((NQ,)),
            DMA((NQ,)),
            DMA((NQ,)),
            DMA((NQ,)),
            DMA,
            DMA((4,)),
            DMA,
            DMA,
            DMA,
            DMA((4,)),
            DMA,
            DMA((4,)),
            DMA,
            DMA,
            pltpu.SemaphoreType.REGULAR((3,)),
        ],
        compiler_params=pltpu.CompilerParams(collective_id=0, has_side_effects=True),
        name="gauss_newton",
    )(src_fields, det_fields, probes)


def solution(mesh):
    return jax.shard_map(
        shards,
        mesh=mesh,
        in_specs=(P("blk", "vox"), P("blk", "vox"), P(None, "vox")),
        out_specs=P(None, "vox"),
        check_vma=False,
    )
```

```python
import functools

import jax
import jax.numpy as jnp
from jax import lax
from jax.experimental import pallas as pl
from jax.experimental.pallas import tpu as pltpu
from jax.sharding import PartitionSpec as P

MESH = pl.DeviceIdType.MESH
BF16 = jnp.bfloat16
F32 = jnp.float32
DMA = pltpu.SemaphoreType.DMA

NX, NY, NZ, NC = 4, 4, 16, 2
NQ = 8
NB = 4


def device(x, y, z, c):
    return (x * 4 + (y // 2) * 2 + c, z * 2 + y % 2)


def send(src, dst, send_sem, recv_sem, to):
    pltpu.make_async_remote_copy(
        src_ref=src, dst_ref=dst, send_sem=send_sem, recv_sem=recv_sem, device_id=to, device_id_type=MESH
    ).start()


def wait_for(ref, sem):
    pltpu.make_async_copy(ref, ref, sem).wait()


def kernel(
    scale,
    src_hbm,
    det_hbm,
    probes_hbm,
    out,
    src_v,
    det_v,
    pr_v,
    pr_in,
    S,
    D,
    acc,
    tx,
    rx,
    zs,
    zr,
    mz,
    M,
    part,
    cv,
    ob,
    ld,
    ysend,
    yS,
    yD,
    pS,
    xsend,
    xS,
    xD,
    c0,
    c1,
    rsend,
    rrecv,
    zsend,
    zrecv,
    gsend,
    grecv,
    asend,
    arecv,
    fsend,
    frecv,
    ready,
):
    blk = lax.axis_index("blk")
    vox = lax.axis_index("vox")
    x, yh, c = blk // 4, (blk // 2) % 2, blk % 2
    z, yl = vox // 2, vox % 2
    y = yh * 2 + yl
    half = src_v.shape[1] // 2
    vc = half // NQ
    scope = jax.named_scope

    up, down = (y + 1) % NY, (y + 3) % NY
    xs = (x // 2) * 2 + 1 - x % 2
    xd = 3 - x
    me = x * 2 + c
    dev_up, dev_down = device(x, up, z, c), device(x, down, z, c)
    dev_xs, dev_xd = device(xs, y, z, c), device(xd, y, z, c)
    dev_c = device(x, y, z, 1 - c)

    def dev_z(d):
        return device(x, y, (z + NZ + d) % NZ, c)

    def signal(sem, to):
        pl.semaphore_signal(sem, inc=1, device_id=to, device_id_type=MESH)

    barrier = pltpu.get_barrier_semaphore()
    near = (dev_up, dev_down, dev_xs, dev_xd, dev_c, dev_z(1), dev_z(-1))
    for to in near:
        signal(barrier, to)

    h_up, h_down = up // 2, down // 2

    parts = [(q, 0, vc) for q in range(NQ - 1)] + [(NQ - 1, 0, vc // 2), (NQ - 1, vc // 2, vc // 2)]

    def columns(h, q, lo, wide):
        return pl.ds(pl.multiple_of(h * half + q * vc + lo, wide), wide)

    pltpu.make_async_copy(probes_hbm, pr_v, ld.at[NQ]).start()
    for q in range(0, NQ, 2):
        for h in range(2):
            at = pl.ds(h * half + q * vc, 2 * vc)
            pltpu.make_async_copy(det_hbm.at[:, at], det_v.at[:, at], ld.at[q]).start()
            pltpu.make_async_copy(src_hbm.at[:, at], src_v.at[:, at], ld.at[q]).start()
    with scope("t_barrier"):
        pl.semaphore_wait(barrier, len(near))

    def spread_word(r):
        d = 2**r
        if r:
            pl.semaphore_wait(ready.at[r - 1], 2)
        if r < 3:
            signal(ready.at[r], dev_z(d))
            signal(ready.at[r], dev_z(-d))

    mine = pl.ds(pl.multiple_of(yh * 64, 64), 64)
    own, other = pl.ds(0, 128), pl.ds(128, 128)
    for n, (q, lo, wide) in enumerate(parts):
        if q % 2 == 0:
            wait_for(D.at[q], ld.at[q])
        to = (q, mine, pl.ds(lo, wide))
        for fields, here, i, sem in ((det_v, D, 0, yD), (src_v, S, 1, yS)):
            send(fields.at[:, columns(h_up, q, lo, wide)], here.at[to], ysend.at[i], sem.at[n], dev_up)
            send(fields.at[:, columns(h_down, q, lo, wide)], here.at[to], ysend.at[i], sem.at[n], dev_down)
        if n == 0:
            wait_for(pr_v, ld.at[NQ])
            send(
                pr_v.at[:, pl.ds(pl.multiple_of(h_up * half, half), half)],
                pr_in,
                ysend.at[2],
                pS,
                dev_up,
            )
            spread_word(0)

    def pass_own(n):
        q, at = parts[n][0], pl.ds(*parts[n][1:])
        wait_for(D.at[q, own, at], yD.at[n])
        send(D.at[q, own, at], D.at[q, other, at], xsend.at[1], xD.at[n], dev_xd)
        send(D.at[q, own, at], D.at[q, pl.ds(256, 128), at], xsend.at[2], c0.at[n], dev_c)
        wait_for(S.at[q, own, at], yS.at[n])
        send(S.at[q, own, at], S.at[q, other, at], xsend.at[0], xS.at[n], dev_xs)

    def pass_other(n):
        q, at = parts[n][0], pl.ds(*parts[n][1:])
        wait_for(D.at[q, other, at], xD.at[n])
        send(D.at[q, other, at], D.at[q, pl.ds(384, 128), at], xsend.at[3], c1.at[n], dev_c)

    def measure(q):
        for n, (of, lo, wide) in enumerate(parts):
            if of == q:
                at = pl.ds(lo, wide)
                wait_for(S.at[q, other, at], xS.at[n])
                wait_for(D.at[q, pl.ds(256, 128), at], c0.at[n])
                wait_for(D.at[q, pl.ds(384, 128), at], c1.at[n])
        fields = S[q].astype(F32)
        p = pr_in[:, q * vc : (q + 1) * vc].astype(F32)
        det = D[q]
        for k in range(2):
            weighted = (fields * p[k : k + 1]).astype(BF16)
            sums = lax.dot_general(weighted, det, (((1,), (1,)), ((), ())), preferred_element_type=F32)
            for g in range(4):
                piece = sums[:, g * 128 : (g + 1) * 128].reshape(4, 2, 32, 128)
                for h in range(2):
                    if q:
                        acc[2 * g + h, :, k] += piece[:, h]
                    else:
                        acc[2 * g + h, :, k] = piece[:, h]

    word = {1: 1, 4: 2}
    for t in range(len(parts) + 4):
        if t < len(parts):
            with scope("g%02d_own" % t):
                pass_own(t)
        if t in word:
            with scope("g%02d_word" % t):
                spread_word(word[t])
        if 0 <= t - 3 < len(parts):
            with scope("g%02d_other" % t):
                pass_other(t - 3)
        if t == 4:
            wait_for(pr_in, pS)
        if 0 <= t - 4 < NQ - 1:
            with scope("g%02d_meas" % t):
                measure(t - 4)
    with scope("g99_meas"):
        measure(NQ - 1)

    pairs = NZ // 2
    zp, zb = z // 2, z % 2
    s = 1 - 2 * zb
    away = (4, 3 * s, -3 * s, 2 * s, -2 * s, s, -s, 0)
    groups = [(zp + pairs + o) % pairs for o in away]
    for i, g in enumerate(groups):
        for d in (2, 1, 3):
            to = (y + d) % NY
            tx[i, to] = acc[g, to].astype(BF16)
            send(tx.at[i, to], rx.at[i, y], rsend, rrecv.at[i], device(x, to, z, c))
    spread_word(3)

    for i, g in enumerate(groups):
        with scope("r%d_y" % i):
            wait_for(rx.at[i, pl.ds(0, 3)], rrecv.at[i])
        total = acc[g, y]
        for d in (1, 2, 3):
            total += rx[i, (y + d) % NY].astype(F32)
        total = total.astype(BF16)
        for k in range(2):
            zs[i, :, k] = total[k].reshape(2, 16, 128)
        if i < pairs - 1:
            for b in (0, 1):
                send(zs.at[i, b], zr.at[z], zsend, zrecv, device(x, y, g * 2 + b, c))
        else:
            send(zs.at[i, 1 - zb], zr.at[z], zsend, zrecv, device(x, y, g * 2 + 1 - zb, c))
    zr[z] = zs[pairs - 1, zb]
    with scope("r_z"):
        wait_for(zr.at[pl.ds(0, NZ - 1)], zrecv)
    total = zr[0].astype(F32)
    for j in range(1, NZ):
        total += zr[j].astype(F32)
    mz[...] = total.astype(BF16)

    M[zp, y, zb] = mz[...]
    for step in range(1, NZ // 2 + 1):
        for to in (step, -step)[: 1 if step == NZ // 2 else 2]:
            send(mz, M.at[zp, y, zb], gsend, grecv.at[zp], dev_z(to))

    back = groups[::-1]
    for i, g in enumerate(back):
        with scope("b%d_z" % i):
            wait_for(zr.at[pl.ds(0, 2 if i else 1)], grecv.at[g])
        for d in (2, 1, 3):
            send(M.at[g, y], M.at[g, y], asend, arecv.at[g], device(x, (y + d) % NY, z, c))

    block, side = zp // 2, 2 * (zp % 2) - 1
    blocks = [(block + o) % 4 for o in (0, 4 + side, 4 - side, 2)]

    def arrived(g):
        for h in range(2):
            wait_for(M.at[2 * g + h, pl.ds(0, 3)], arecv.at[2 * g + h])

    def contribution(q, lo):
        two = blocks[lo : lo + 2]
        lhs = jnp.concatenate([M[pl.ds(2 * g, 2)].reshape(512, 128) for g in two], axis=1)
        det = jnp.concatenate([D[q, pl.ds(pl.multiple_of(g * 128, 128), 128)] for g in two], axis=0)
        bp = jnp.dot(lhs, det, preferred_element_type=F32).reshape(2, 4, 2, 2, 16, vc)
        fields = S[q].astype(F32).reshape(4, 2, 2, 16, vc)
        sums = []
        for k in range(2):
            row = jnp.zeros((8, vc), F32)
            for h in range(2):
                for b in range(2):
                    row += jnp.sum((fields[:, h, b] * bp[h, :, b, k]).reshape(8, 8, vc), axis=0)
            sums.append(row)
        return sums

    arrived(blocks[0])
    with scope("b1_y"):
        arrived(blocks[1])
    with scope("m_front"):
        for q in range(NQ):
            part[q, 0], part[q, 1] = contribution(q, 0)
    with scope("b2_y"):
        arrived(blocks[2])
    with scope("b3_y"):
        arrived(blocks[3])

    per = NQ // NB
    with scope("m_rest"):
        for n in range(NB):
            rows = [[], []]
            for q in range(n * per, (n + 1) * per):
                for k, sums in enumerate(contribution(q, 2)):
                    row = jnp.sum(part[q, k] + sums, axis=0, keepdims=True)
                    rows[k] += [row[:, i * 128 : (i + 1) * 128] for i in range(vc // 128)]
            cv[n] = jnp.concatenate(rows[0] + rows[1], axis=0).reshape(-1, 8, 128)
            for e in range(NX * NC):
                for to in (up, down):
                    send(cv.at[n], ob.at[yh, me, n], fsend, frecv, device(e // 2, to, z, e % 2))
    with scope("f_recv"):
        wait_for(ob, frecv)
    wide = half // NB
    for h in range(2):
        for n in range(NB):
            whole = ob[h, 0, n]
            for e in range(1, NX * NC):
                whole += ob[h, e, n]
            whole = (whole * scale).reshape(-1, 128)
            for k in range(2):
                for i in range(wide // 128):
                    at = h * half + n * wide + i * 128
                    row = k * (wide // 128) + i
                    out[k : k + 1, at : at + 128] = whole[row : row + 1]

    wait_for(det_v, ysend.at[0])
    wait_for(src_v, ysend.at[1])
    wait_for(pr_in, ysend.at[2])
    wait_for(S.at[:, own], xsend.at[0])
    for i in (1, 2, 3):
        wait_for(D.at[:, own], xsend.at[i])
    wait_for(tx.at[:, pl.ds(0, 3)], rsend)
    wait_for(zr.at[pl.ds(0, NZ - 1)], zsend)
    wait_for(zr.at[pl.ds(0, NZ - 1)], gsend)
    wait_for(M.at[:, pl.ds(0, 3)], asend)
    wait_for(ob, fsend)


def shards(src_fields, det_fields, probes):
    rows, voxels = src_fields.shape
    half = voxels // 2
    vc = half // NQ
    sources, detectors = rows * lax.axis_size("blk"), det_fields.shape[0] * lax.axis_size("blk")
    scale = 1.0 / (sources * detectors)
    hbm = pl.BlockSpec(memory_space=pl.ANY)
    return pl.pallas_call(
        functools.partial(kernel, scale),
        out_shape=jax.ShapeDtypeStruct((2, voxels), F32),
        in_specs=[hbm] * 3,
        out_specs=pl.BlockSpec(memory_space=pltpu.VMEM),
        scratch_shapes=[
            pltpu.VMEM((64, voxels), BF16),
            pltpu.VMEM((64, voxels), BF16),
            pltpu.VMEM((2, voxels), BF16),
            pltpu.VMEM((2, half), BF16),
            pltpu.VMEM((NQ, 256, vc), BF16),
            pltpu.VMEM((NQ, 512, vc), BF16),
            pltpu.VMEM((8, 4, 2, 32, 128), F32),
            pltpu.VMEM((8, 4, 2, 32, 128), BF16),
            pltpu.VMEM((8, 4, 2, 32, 128), BF16),
            pltpu.VMEM((8, 2, 2, 16, 128), BF16),
            pltpu.VMEM((NZ, 2, 16, 128), BF16),
            pltpu.VMEM((2, 16, 128), BF16),
            pltpu.VMEM((8, 4, 2, 2, 16, 128), BF16),
            pltpu.VMEM((NQ, 2, 8, vc), F32),
            pltpu.VMEM((NB, half // NB // 512, 8, 128), F32),
            pltpu.VMEM((2, NX * NC, NB, half // NB // 512, 8, 128), F32),
            DMA((NQ + 1,)),
            DMA((3,)),
            DMA((NQ + 1,)),
            DMA((NQ + 1,)),
            DMA,
            DMA((4,)),
            DMA((NQ + 1,)),
            DMA((NQ + 1,)),
            DMA((NQ + 1,)),
            DMA((NQ + 1,)),
            DMA,
            DMA((8,)),
            DMA,
            DMA,
            DMA,
            DMA((8,)),
            DMA,
            DMA((8,)),
            DMA,
            DMA,
            pltpu.SemaphoreType.REGULAR((3,)),
        ],
        compiler_params=pltpu.CompilerParams(
            collective_id=0, has_side_effects=True, vmem_limit_bytes=60 * 2**20
        ),
        name="gauss_newton",
    )(src_fields, det_fields, probes)


def solution(mesh):
    return jax.shard_map(
        shards,
        mesh=mesh,
        in_specs=(P("blk", "vox"), P("blk", "vox"), P(None, "vox")),
        out_specs=P(None, "vox"),
        check_vma=False,
    )
```

```python
import functools

import jax
import jax.numpy as jnp
from jax import lax
from jax.experimental import pallas as pl
from jax.experimental.pallas import tpu as pltpu
from jax.sharding import PartitionSpec as P

MESH = pl.DeviceIdType.MESH
BF16 = jnp.bfloat16
F32 = jnp.float32
DMA = pltpu.SemaphoreType.DMA

NX, NY, NZ, NC = 4, 4, 16, 2
NQ = 8
NB = 2


def device(x, y, z, c):
    return (x * 4 + (y // 2) * 2 + c, z * 2 + y % 2)


def send(src, dst, send_sem, recv_sem, to):
    pltpu.make_async_remote_copy(
        src_ref=src, dst_ref=dst, send_sem=send_sem, recv_sem=recv_sem, device_id=to, device_id_type=MESH
    ).start()


def wait_for(ref, sem):
    pltpu.make_async_copy(ref, ref, sem).wait()


def kernel(
    scale,
    src_hbm,
    det_hbm,
    probes_hbm,
    out,
    src_v,
    det_v,
    pr_v,
    pr_in,
    S,
    D,
    acc,
    tx,
    rx,
    zs,
    zr,
    mz,
    M,
    part,
    cv,
    ob,
    ld,
    ysend,
    yS,
    yD,
    pS,
    xsend,
    xS,
    xD,
    c0,
    c1,
    rsend,
    rrecv,
    zsend,
    zrecv,
    gsend,
    grecv,
    asend,
    arecv,
    fsend,
    frecv,
    ready,
):
    blk = lax.axis_index("blk")
    vox = lax.axis_index("vox")
    x, yh, c = blk // 4, (blk // 2) % 2, blk % 2
    z, yl = vox // 2, vox % 2
    y = yh * 2 + yl
    half = src_v.shape[1] // 2
    vc = half // NQ
    scope = jax.named_scope

    up, down = (y + 1) % NY, (y + 3) % NY
    xs = (x // 2) * 2 + 1 - x % 2
    xd = 3 - x
    me = x * 2 + c
    dev_up, dev_down = device(x, up, z, c), device(x, down, z, c)
    dev_xs, dev_xd = device(xs, y, z, c), device(xd, y, z, c)
    dev_c = device(x, y, z, 1 - c)

    def dev_z(d):
        return device(x, y, (z + NZ + d) % NZ, c)

    def signal(sem, to):
        pl.semaphore_signal(sem, inc=1, device_id=to, device_id_type=MESH)

    barrier = pltpu.get_barrier_semaphore()
    near = (dev_up, dev_down, dev_xs, dev_xd, dev_c, dev_z(1), dev_z(-1))
    for to in near:
        signal(barrier, to)

    h_up, h_down = up // 2, down // 2

    parts = [(q, 0, vc) for q in range(NQ - 1)] + [(NQ - 1, 0, vc // 2), (NQ - 1, vc // 2, vc // 2)]

    def columns(h, q, lo, wide):
        return pl.ds(pl.multiple_of(h * half + q * vc + lo, wide), wide)

    pltpu.make_async_copy(probes_hbm, pr_v, ld.at[NQ]).start()
    for q in range(0, NQ, 2):
        for h in range(2):
            at = pl.ds(h * half + q * vc, 2 * vc)
            pltpu.make_async_copy(det_hbm.at[:, at], det_v.at[:, at], ld.at[q]).start()
            pltpu.make_async_copy(src_hbm.at[:, at], src_v.at[:, at], ld.at[q + 1]).start()
    with scope("t_barrier"):
        pl.semaphore_wait(barrier, len(near))

    def spread_word(r):
        d = 2**r
        if r:
            pl.semaphore_wait(ready.at[r - 1], 2)
        if r < 3:
            signal(ready.at[r], dev_z(d))
            signal(ready.at[r], dev_z(-d))

    mine = pl.ds(pl.multiple_of(yh * 64, 64), 64)
    own, other = pl.ds(0, 128), pl.ds(128, 128)
    LEAD = 2
    last = len(parts)

    def swap(fields, here, i, sem, n):
        q, lo, wide = parts[n]
        if q % 2 == 0:
            wait_for(D.at[q, pl.ds(0, 256)], ld.at[q + i])
        to = (q, mine, pl.ds(lo, wide))
        send(fields.at[:, columns(h_up, q, lo, wide)], here.at[to], ysend.at[i], sem.at[n], dev_up)
        send(fields.at[:, columns(h_down, q, lo, wide)], here.at[to], ysend.at[i], sem.at[n], dev_down)

    for t in range(last + LEAD):
        if t < last:
            swap(det_v, D, 0, yD, t)
        if t >= LEAD:
            swap(src_v, S, 1, yS, t - LEAD)
        if t == 0:
            wait_for(pr_v, ld.at[NQ])
            send(
                pr_v.at[:, pl.ds(pl.multiple_of(h_up * half, half), half)],
                pr_in,
                ysend.at[2],
                pS,
                dev_up,
            )
            spread_word(0)

    def pass_det(n):
        q, at = parts[n][0], pl.ds(*parts[n][1:])
        wait_for(D.at[q, own, at], yD.at[n])
        send(D.at[q, own, at], D.at[q, other, at], xsend.at[1], xD.at[n], dev_xd)
        send(D.at[q, own, at], D.at[q, pl.ds(256, 128), at], xsend.at[2], c0.at[n], dev_c)

    def pass_src(n):
        q, at = parts[n][0], pl.ds(*parts[n][1:])
        wait_for(S.at[q, own, at], yS.at[n])
        send(S.at[q, own, at], S.at[q, other, at], xsend.at[0], xS.at[n], dev_xs)

    def pass_other(n):
        q, at = parts[n][0], pl.ds(*parts[n][1:])
        wait_for(D.at[q, other, at], xD.at[n])
        send(D.at[q, other, at], D.at[q, pl.ds(384, 128), at], xsend.at[3], c1.at[n], dev_c)

    def measure(n):
        q, lo, wide = parts[n]
        at = pl.ds(lo, wide)
        wait_for(D.at[q, pl.ds(256, 128), at], c0.at[n])
        wait_for(D.at[q, pl.ds(384, 128), at], c1.at[n])
        wait_for(S.at[q, other, at], xS.at[n])
        fields = S[q, :, at].astype(F32)
        p = pr_in[:, q * vc + lo : q * vc + lo + wide].astype(F32)
        det = D[q, :, at]
        for k in range(2):
            weighted = (fields * p[k : k + 1]).astype(BF16)
            sums = lax.dot_general(weighted, det, (((1,), (1,)), ((), ())), preferred_element_type=F32)
            for g in range(4):
                piece = sums[:, g * 128 : (g + 1) * 128].reshape(4, 2, 32, 128)
                for h in range(2):
                    if n:
                        acc[k, 2 * g + h] += piece[:, h]
                    else:
                        acc[k, 2 * g + h] = piece[:, h]

    word = {1: 1, 4: 2}
    for t in range(last + 5):
        if t < last:
            with scope("g%02d_det" % t):
                pass_det(t)
        if 0 <= t - LEAD < last:
            with scope("g%02d_src" % t):
                pass_src(t - LEAD)
        if t in word:
            with scope("g%02d_word" % t):
                spread_word(word[t])
        if 0 <= t - 3 < last:
            with scope("g%02d_other" % t):
                pass_other(t - 3)
        if t == 5:
            wait_for(pr_in, pS)
        if 0 <= t - 5 < last:
            with scope("g%02d_meas" % t):
                measure(t - 5)

    pairs = NZ // 2
    zp, zb = z // 2, z % 2
    s = 1 - 2 * zb
    away = (4, 3 * s, -3 * s, 2 * s, -2 * s, s, -s, 0)
    groups = [(zp + pairs + o) % pairs for o in away]
    for k in range(2):
        for i, g in enumerate(groups):
            for d in (2, 1, 3):
                to = (y + d) % NY
                tx[k, i, to] = acc[k, g, to].astype(BF16)
                send(tx.at[k, i, to], rx.at[k, i, y], rsend, rrecv.at[k, i], device(x, to, z, c))
    spread_word(3)

    def along_z(k):
        for i, g in enumerate(groups):
            with scope("r%d%d_y" % (k, i)):
                wait_for(rx.at[k, i, pl.ds(0, 3)], rrecv.at[k, i])
            total = acc[k, g, y]
            for d in (1, 2, 3):
                total += rx[k, i, (y + d) % NY].astype(F32)
            zs[k, i] = total.astype(BF16).reshape(2, 16, 128)
            for b in (0, 1) if i < pairs - 1 else (1 - zb,):
                send(zs.at[k, i, b], zr.at[k, z], zsend, zrecv.at[k], device(x, y, g * 2 + b, c))
        zr[k, z] = zs[k, pairs - 1, zb]

    def back_along_z(k):
        with scope("r%d_z" % k):
            wait_for(zr.at[k, pl.ds(0, NZ - 1)], zrecv.at[k])
        total = zr[k, 0].astype(F32)
        for j in range(1, NZ):
            total += zr[k, j].astype(F32)
        mz[k] = total.astype(BF16)
        M[k, zp, y, zb] = mz[k]
        for step in range(NZ // 2, 0, -1):
            for to in (step, -step)[: 1 if step == NZ // 2 else 2]:
                send(mz.at[k], M.at[k, zp, y, zb], gsend, grecv.at[k, zp], dev_z(to))

    back = groups[::-1]

    def back_along_y(k):
        for i, g in enumerate(back):
            with scope("b%d%d_z" % (k, i)):
                wait_for(zr.at[k, pl.ds(0, 2 if i else 1)], grecv.at[k, g])
            for d in (2, 1, 3):
                send(M.at[k, g, y], M.at[k, g, y], asend, arecv.at[k, g], device(x, (y + d) % NY, z, c))

    block, side = zp // 2, 2 * (zp % 2) - 1
    blocks = [(block + o) % 4 for o in (0, 4 + side, 4 - side, 2)]

    def arrived(k, g):
        for h in range(2):
            wait_for(M.at[k, 2 * g + h, pl.ds(0, 3)], arecv.at[k, 2 * g + h])

    def contribution(k, q, lo):
        two = blocks[lo : lo + 2]
        lhs = jnp.concatenate([M[k, pl.ds(2 * g, 2)].reshape(256, 128) for g in two], axis=1)
        det = jnp.concatenate([D[q, pl.ds(pl.multiple_of(g * 128, 128), 128)] for g in two], axis=0)
        bp = jnp.dot(lhs, det, preferred_element_type=F32).reshape(2, 4, 32, vc)
        fields = S[q].astype(F32).reshape(4, 2, 32, vc)
        row = jnp.zeros((8, vc), F32)
        for h in range(2):
            row += jnp.sum((fields[:, h] * bp[h]).reshape(16, 8, vc), axis=0)
        return row

    def front(k):
        with scope("m%d_front" % k):
            arrived(k, blocks[0])
            arrived(k, blocks[1])
            for q in range(NQ):
                part[k, q] = contribution(k, q, 0)

    def rest(k):
        with scope("m%d_y" % k):
            arrived(k, blocks[2])
            arrived(k, blocks[3])
        per = NQ // NB
        with scope("m%d_rest" % k):
            for n in range(NB):
                rows = []
                for q in range(n * per, (n + 1) * per):
                    row = jnp.sum(part[k, q] + contribution(k, q, 2), axis=0, keepdims=True)
                    rows += [row[:, i * 128 : (i + 1) * 128] for i in range(vc // 128)]
                cv[k, n] = jnp.concatenate(rows, axis=0)
                for e in range(NX * NC):
                    for to in (up, down):
                        send(cv.at[k, n], ob.at[k, yh, me, n], fsend, frecv.at[k], device(e // 2, to, z, e % 2))

    def finish(k):
        with scope("f%d_recv" % k):
            wait_for(ob.at[k], frecv.at[k])
        wide = half // NB
        for h in range(2):
            for n in range(NB):
                whole = ob[k, h, 0, n]
                for e in range(1, NX * NC):
                    whole += ob[k, h, e, n]
                whole = whole * scale
                for i in range(wide // 128):
                    at = h * half + n * wide + i * 128
                    out[k : k + 1, at : at + 128] = whole[i : i + 1]

    along_z(0)
    along_z(1)
    back_along_z(0)
    back_along_z(1)
    back_along_y(0)
    back_along_y(1)
    front(0)
    rest(0)
    front(1)
    rest(1)
    finish(0)
    finish(1)

    wait_for(det_v, ysend.at[0])
    wait_for(src_v, ysend.at[1])
    wait_for(pr_in, ysend.at[2])
    wait_for(S.at[:, own], xsend.at[0])
    for i in (1, 2, 3):
        wait_for(D.at[:, own], xsend.at[i])
    wait_for(tx.at[:, :, pl.ds(0, 3)], rsend)
    wait_for(zr.at[:, pl.ds(0, NZ - 1)], zsend)
    wait_for(zr.at[:, pl.ds(0, NZ - 1)], gsend)
    wait_for(M.at[:, :, pl.ds(0, 3)], asend)
    wait_for(ob, fsend)


def shards(src_fields, det_fields, probes):
    rows, voxels = src_fields.shape
    half = voxels // 2
    vc = half // NQ
    sources, detectors = rows * lax.axis_size("blk"), det_fields.shape[0] * lax.axis_size("blk")
    scale = 1.0 / (sources * detectors)
    hbm = pl.BlockSpec(memory_space=pl.ANY)
    return pl.pallas_call(
        functools.partial(kernel, scale),
        out_shape=jax.ShapeDtypeStruct((2, voxels), F32),
        in_specs=[hbm] * 3,
        out_specs=pl.BlockSpec(memory_space=pltpu.VMEM),
        scratch_shapes=[
            pltpu.VMEM((64, voxels), BF16),
            pltpu.VMEM((64, voxels), BF16),
            pltpu.VMEM((2, voxels), BF16),
            pltpu.VMEM((2, half), BF16),
            pltpu.VMEM((NQ, 256, vc), BF16),
            pltpu.VMEM((NQ, 512, vc), BF16),
            pltpu.VMEM((2, 8, 4, 32, 128), F32),
            pltpu.VMEM((2, 8, 4, 32, 128), BF16),
            pltpu.VMEM((2, 8, 4, 32, 128), BF16),
            pltpu.VMEM((2, 8, 2, 16, 128), BF16),
            pltpu.VMEM((2, NZ, 16, 128), BF16),
            pltpu.VMEM((2, 16, 128), BF16),
            pltpu.VMEM((2, 8, 4, 2, 16, 128), BF16),
            pltpu.VMEM((2, NQ, 8, vc), F32),
            pltpu.VMEM((2, NB, half // NB // 128, 128), F32),
            pltpu.VMEM((2, 2, NX * NC, NB, half // NB // 128, 128), F32),
            DMA((NQ + 1,)),
            DMA((3,)),
            DMA((NQ + 1,)),
            DMA((NQ + 1,)),
            DMA,
            DMA((4,)),
            DMA((NQ + 1,)),
            DMA((NQ + 1,)),
            DMA((NQ + 1,)),
            DMA((NQ + 1,)),
            DMA,
            DMA((2, 8)),
            DMA,
            DMA((2,)),
            DMA,
            DMA((2, 8)),
            DMA,
            DMA((2, 8)),
            DMA,
            DMA((2,)),
            pltpu.SemaphoreType.REGULAR((3,)),
        ],
        compiler_params=pltpu.CompilerParams(
            collective_id=0, has_side_effects=True, vmem_limit_bytes=60 * 2**20
        ),
        name="gauss_newton",
    )(src_fields, det_fields, probes)


def solution(mesh):
    return jax.shard_map(
        shards,
        mesh=mesh,
        in_specs=(P("blk", "vox"), P("blk", "vox"), P(None, "vox")),
        out_specs=P(None, "vox"),
        check_vma=False,
    )
```

```python
import functools

import jax
import jax.numpy as jnp
from jax import lax
from jax.experimental import pallas as pl
from jax.experimental.pallas import tpu as pltpu
from jax.sharding import PartitionSpec as P

MESH = pl.DeviceIdType.MESH
BF16 = jnp.bfloat16
F32 = jnp.float32
DMA = pltpu.SemaphoreType.DMA

NX, NY, NZ, NC = 4, 4, 16, 2
NQ = 8
NB = 2


def device(x, y, z, c):
    return (x * 4 + (y // 2) * 2 + c, z * 2 + y % 2)


def send(src, dst, send_sem, recv_sem, to):
    pltpu.make_async_remote_copy(
        src_ref=src, dst_ref=dst, send_sem=send_sem, recv_sem=recv_sem, device_id=to, device_id_type=MESH
    ).start()


def wait_for(ref, sem):
    pltpu.make_async_copy(ref, ref, sem).wait()


def kernel(
    scale,
    src_hbm,
    det_hbm,
    probes_hbm,
    out,
    src_v,
    det_v,
    pr_v,
    pr_in,
    S,
    D,
    acc,
    tx,
    rx,
    zs,
    zr,
    mz,
    M,
    part,
    cv,
    ob,
    ld,
    ysend,
    yS,
    yD,
    pS,
    xsend,
    xS,
    xD,
    c0,
    c1,
    rsend,
    rrecv,
    zsend,
    zrecv,
    gsend,
    grecv,
    asend,
    arecv,
    fsend,
    frecv,
    ready,
):
    blk = lax.axis_index("blk")
    vox = lax.axis_index("vox")
    x, yh, c = blk // 4, (blk // 2) % 2, blk % 2
    z, yl = vox // 2, vox % 2
    y = yh * 2 + yl
    half = src_v.shape[1] // 2
    vc = half // NQ
    scope = jax.named_scope

    up, down = (y + 1) % NY, (y + 3) % NY
    xs = (x // 2) * 2 + 1 - x % 2
    xd = 3 - x
    me = x * 2 + c
    dev_up, dev_down = device(x, up, z, c), device(x, down, z, c)
    dev_xs, dev_xd = device(xs, y, z, c), device(xd, y, z, c)
    dev_c = device(x, y, z, 1 - c)

    def dev_z(d):
        return device(x, y, (z + NZ + d) % NZ, c)

    def signal(sem, to):
        pl.semaphore_signal(sem, inc=1, device_id=to, device_id_type=MESH)

    barrier = pltpu.get_barrier_semaphore()
    near = (dev_up, dev_down, dev_xs, dev_xd, dev_c, dev_z(1), dev_z(-1))
    for to in near:
        signal(barrier, to)

    h_up, h_down = up // 2, down // 2

    parts = []
    for q in range(NQ):
        cuts = 2 if q in (0, NQ - 1) else 1
        parts += [(q, i * vc // cuts, vc // cuts) for i in range(cuts)]
    last = len(parts)

    def columns(h, q, lo, wide):
        return pl.ds(pl.multiple_of(h * half + q * vc + lo, wide), wide)

    pltpu.make_async_copy(probes_hbm, pr_v, ld.at[NQ]).start()
    for q in range(0, NQ, 2):
        for h in range(2):
            at = pl.ds(h * half + q * vc, 2 * vc)
            pltpu.make_async_copy(det_hbm.at[:, at], det_v.at[:, at], ld.at[q]).start()
            pltpu.make_async_copy(src_hbm.at[:, at], src_v.at[:, at], ld.at[q + 1]).start()
    with scope("t_barrier"):
        pl.semaphore_wait(barrier, len(near))

    def spread_word(r):
        d = 2**r
        if r:
            pl.semaphore_wait(ready.at[r - 1], 2)
        if r < 3:
            signal(ready.at[r], dev_z(d))
            signal(ready.at[r], dev_z(-d))

    mine = pl.ds(pl.multiple_of(yh * 64, 64), 64)
    own, other = pl.ds(0, 128), pl.ds(128, 128)
    def swap(fields, here, i, sem, n):
        q, lo, wide = parts[n]
        if q % 2 == 0 and lo == 0:
            wait_for(D.at[q, pl.ds(0, 256)], ld.at[q + i])
        to = (q, mine, pl.ds(lo, wide))
        send(fields.at[:, columns(h_up, q, lo, wide)], here.at[to], ysend.at[i], sem.at[n], dev_up)
        send(fields.at[:, columns(h_down, q, lo, wide)], here.at[to], ysend.at[i], sem.at[n], dev_down)

    for t in range(last):
        swap(det_v, D, 0, yD, t)
        swap(src_v, S, 1, yS, t)
        if t == 0:
            wait_for(pr_v, ld.at[NQ])
            send(
                pr_v.at[:, pl.ds(pl.multiple_of(h_up * half, half), half)],
                pr_in,
                ysend.at[2],
                pS,
                dev_up,
            )
            spread_word(0)

    def pass_own(n):
        q, at = parts[n][0], pl.ds(*parts[n][1:])
        wait_for(D.at[q, own, at], yD.at[n])
        send(D.at[q, own, at], D.at[q, other, at], xsend.at[1], xD.at[n], dev_xd)
        send(D.at[q, own, at], D.at[q, pl.ds(256, 128), at], xsend.at[2], c0.at[n], dev_c)
        if n == last - 1:
            send(D.at[q, own, at], D.at[q, pl.ds(384, 128), at], xsend.at[3], c1.at[n], device(xd, y, z, 1 - c))
        wait_for(S.at[q, own, at], yS.at[n])
        send(S.at[q, own, at], S.at[q, other, at], xsend.at[0], xS.at[n], dev_xs)

    def pass_other(n):
        q, at = parts[n][0], pl.ds(*parts[n][1:])
        wait_for(D.at[q, other, at], xD.at[n])
        if n < last - 1:
            send(D.at[q, other, at], D.at[q, pl.ds(384, 128), at], xsend.at[3], c1.at[n], dev_c)

    def measure(n):
        q, lo, wide = parts[n]
        at = pl.ds(lo, wide)
        wait_for(D.at[q, pl.ds(256, 128), at], c0.at[n])
        wait_for(D.at[q, pl.ds(384, 128), at], c1.at[n])
        wait_for(S.at[q, other, at], xS.at[n])
        fields = S[q, :, at].astype(F32)
        p = pr_in[:, q * vc + lo : q * vc + lo + wide].astype(F32)
        det = D[q, :, at]
        for k in range(2):
            weighted = (fields * p[k : k + 1]).astype(BF16)
            sums = lax.dot_general(weighted, det, (((1,), (1,)), ((), ())), preferred_element_type=F32)
            for g in range(4):
                piece = sums[:, g * 128 : (g + 1) * 128].reshape(4, 2, 32, 128)
                for h in range(2):
                    if n:
                        acc[k, 2 * g + h] += piece[:, h]
                    else:
                        acc[k, 2 * g + h] = piece[:, h]

    word = {3: 1, 6: 2}
    for t in range(last + 6):
        if t < last:
            with scope("g%02d_own" % t):
                pass_own(t)
        if t in word:
            with scope("g%02d_word" % t):
                spread_word(word[t])
        if 0 <= t - 4 < last:
            with scope("g%02d_other" % t):
                pass_other(t - 4)
        if t == 6:
            wait_for(pr_in, pS)
        if 0 <= t - 6 < last:
            with scope("g%02d_meas" % t):
                measure(t - 6)

    pairs = NZ // 2
    zp, zb = z // 2, z % 2
    s = 1 - 2 * zb
    away = (4, 3 * s, -3 * s, 2 * s, -2 * s, s, -s, 0)
    groups = [(zp + pairs + o) % pairs for o in away]
    turns = [(0, 0), (0, 1), (0, 2), (1, 0), (1, 1), (1, 2), (0, 3), (0, 4), (1, 3), (1, 4)]
    turns += [(0, 5), (0, 6), (0, 7), (1, 5), (1, 6), (1, 7)]
    for k, i in turns:
        for d in (2, 1, 3):
            to = (y + d) % NY
            tx[k, i, to] = acc[k, groups[i], to].astype(BF16)
            send(tx.at[k, i, to], rx.at[k, i, y], rsend, rrecv.at[k, i], device(x, to, z, c))
    spread_word(3)

    for k, i in turns:
        g = groups[i]
        with scope("r%d%d_y" % (k, i)):
            wait_for(rx.at[k, i, pl.ds(0, 3)], rrecv.at[k, i])
        total = acc[k, g, y]
        for d in (1, 2, 3):
            total += rx[k, i, (y + d) % NY].astype(F32)
        zs[k, i] = total.astype(BF16).reshape(2, 16, 128)
        for b in (0, 1) if i < pairs - 1 else (1 - zb,):
            send(zs.at[k, i, b], zr.at[k, z], zsend, zrecv.at[k], device(x, y, g * 2 + b, c))
    for k in range(2):
        zr[k, z] = zs[k, pairs - 1, zb]

    def back_along_z(k):
        with scope("r%d_z" % k):
            wait_for(zr.at[k, pl.ds(0, NZ - 1)], zrecv.at[k])
        total = zr[k, 0].astype(F32)
        for j in range(1, NZ):
            total += zr[k, j].astype(F32)
        mz[k] = total.astype(BF16)
        M[k, zp, y, zb] = mz[k]
        for step in range(NZ // 2, 0, -1):
            for to in (step, -step)[: 1 if step == NZ // 2 else 2]:
                send(mz.at[k], M.at[k, zp, y, zb], gsend, grecv.at[k, zp], dev_z(to))

    back = groups[::-1]

    def back_along_y(k):
        for i, g in enumerate(back):
            with scope("b%d%d_z" % (k, i)):
                wait_for(zr.at[k, pl.ds(0, 2 if i else 1)], grecv.at[k, g])
            for d in (2, 1, 3):
                send(M.at[k, g, y], M.at[k, g, y], asend, arecv.at[k, g], device(x, (y + d) % NY, z, c))

    block, side = zp // 2, 2 * (zp % 2) - 1
    blocks = [(block + o) % 4 for o in (0, 4 + side, 4 - side, 2)]

    def arrived(k, g):
        for h in range(2):
            wait_for(M.at[k, 2 * g + h, pl.ds(0, 3)], arecv.at[k, 2 * g + h])

    def contribution(k, q, lo):
        two = blocks[lo : lo + 2]
        lhs = jnp.concatenate([M[k, pl.ds(2 * g, 2)].reshape(256, 128) for g in two], axis=1)
        det = jnp.concatenate([D[q, pl.ds(pl.multiple_of(g * 128, 128), 128)] for g in two], axis=0)
        bp = jnp.dot(lhs, det, preferred_element_type=F32).reshape(2, 4, 32, vc)
        fields = S[q].astype(F32).reshape(4, 2, 32, vc)
        row = jnp.zeros((8, vc), F32)
        for h in range(2):
            row += jnp.sum((fields[:, h] * bp[h]).reshape(16, 8, vc), axis=0)
        return row

    def front(k):
        with scope("m%d_front" % k):
            arrived(k, blocks[0])
            arrived(k, blocks[1])
            for q in range(NQ):
                part[k, q] = contribution(k, q, 0)

    def rest(k):
        with scope("m%d_y" % k):
            arrived(k, blocks[2])
            arrived(k, blocks[3])
        per = NQ // NB
        with scope("m%d_rest" % k):
            for n in range(NB):
                rows = []
                for q in range(n * per, (n + 1) * per):
                    row = jnp.sum(part[k, q] + contribution(k, q, 2), axis=0, keepdims=True)
                    rows += [row[:, i * 128 : (i + 1) * 128] for i in range(vc // 128)]
                cv[k, n] = jnp.concatenate(rows, axis=0)
                for e in range(NX * NC):
                    for to in (up, down):
                        send(cv.at[k, n], ob.at[k, yh, me, n], fsend, frecv.at[k], device(e // 2, to, z, e % 2))

    def finish(k):
        with scope("f%d_recv" % k):
            wait_for(ob.at[k], frecv.at[k])
        wide = half // NB
        for h in range(2):
            for n in range(NB):
                whole = ob[k, h, 0, n]
                for e in range(1, NX * NC):
                    whole += ob[k, h, e, n]
                whole = whole * scale
                for i in range(wide // 128):
                    at = h * half + n * wide + i * 128
                    out[k : k + 1, at : at + 128] = whole[i : i + 1]

    back_along_z(0)
    back_along_z(1)
    back_along_y(0)
    back_along_y(1)
    front(0)
    rest(0)
    front(1)
    rest(1)
    finish(0)
    finish(1)

    wait_for(det_v, ysend.at[0])
    wait_for(src_v, ysend.at[1])
    wait_for(pr_in, ysend.at[2])
    wait_for(S.at[:, own], xsend.at[0])
    for i in (1, 2, 3):
        wait_for(D.at[:, own], xsend.at[i])
    wait_for(tx.at[:, :, pl.ds(0, 3)], rsend)
    wait_for(zr.at[:, pl.ds(0, NZ - 1)], zsend)
    wait_for(zr.at[:, pl.ds(0, NZ - 1)], gsend)
    wait_for(M.at[:, :, pl.ds(0, 3)], asend)
    wait_for(ob, fsend)


def shards(src_fields, det_fields, probes):
    rows, voxels = src_fields.shape
    half = voxels // 2
    vc = half // NQ
    sources, detectors = rows * lax.axis_size("blk"), det_fields.shape[0] * lax.axis_size("blk")
    scale = 1.0 / (sources * detectors)
    hbm = pl.BlockSpec(memory_space=pl.ANY)
    given = [pltpu.with_memory_space_constraint(a, pltpu.HBM) for a in (src_fields, det_fields, probes)]
    return pl.pallas_call(
        functools.partial(kernel, scale),
        out_shape=jax.ShapeDtypeStruct((2, voxels), F32),
        in_specs=[hbm] * 3,
        out_specs=pl.BlockSpec(memory_space=pltpu.VMEM),
        scratch_shapes=[
            pltpu.VMEM((64, voxels), BF16),
            pltpu.VMEM((64, voxels), BF16),
            pltpu.VMEM((2, voxels), BF16),
            pltpu.VMEM((2, half), BF16),
            pltpu.VMEM((NQ, 256, vc), BF16),
            pltpu.VMEM((NQ, 512, vc), BF16),
            pltpu.VMEM((2, 8, 4, 32, 128), F32),
            pltpu.VMEM((2, 8, 4, 32, 128), BF16),
            pltpu.VMEM((2, 8, 4, 32, 128), BF16),
            pltpu.VMEM((2, 8, 2, 16, 128), BF16),
            pltpu.VMEM((2, NZ, 16, 128), BF16),
            pltpu.VMEM((2, 16, 128), BF16),
            pltpu.VMEM((2, 8, 4, 2, 16, 128), BF16),
            pltpu.VMEM((2, NQ, 8, vc), F32),
            pltpu.VMEM((2, NB, half // NB // 128, 128), F32),
            pltpu.VMEM((2, 2, NX * NC, NB, half // NB // 128, 128), F32),
            DMA((NQ + 1,)),
            DMA((3,)),
            DMA((NQ + 2,)),
            DMA((NQ + 2,)),
            DMA,
            DMA((4,)),
            DMA((NQ + 2,)),
            DMA((NQ + 2,)),
            DMA((NQ + 2,)),
            DMA((NQ + 2,)),
            DMA,
            DMA((2, 8)),
            DMA,
            DMA((2,)),
            DMA,
            DMA((2, 8)),
            DMA,
            DMA((2, 8)),
            DMA,
            DMA((2,)),
            pltpu.SemaphoreType.REGULAR((3,)),
        ],
        compiler_params=pltpu.CompilerParams(
            collective_id=0, has_side_effects=True, vmem_limit_bytes=50_000_000
        ),
        name="gauss_newton",
    )(*given)


def solution(mesh):
    return jax.shard_map(
        shards,
        mesh=mesh,
        in_specs=(P("blk", "vox"), P("blk", "vox"), P(None, "vox")),
        out_specs=P(None, "vox"),
        check_vma=False,
    )
```

```python
import functools

import jax
import jax.numpy as jnp
from jax import lax
from jax.experimental import pallas as pl
from jax.experimental.pallas import tpu as pltpu
from jax.sharding import PartitionSpec as P

MESH = pl.DeviceIdType.MESH
BF16 = jnp.bfloat16
F32 = jnp.float32
DMA = pltpu.SemaphoreType.DMA

NX, NY, NZ, NC = 4, 4, 16, 2
NQ = 8
NB = 2


def device(x, y, z, c):
    return (x * 4 + (y // 2) * 2 + c, z * 2 + y % 2)


def send(src, dst, send_sem, recv_sem, to):
    pltpu.make_async_remote_copy(
        src_ref=src, dst_ref=dst, send_sem=send_sem, recv_sem=recv_sem, device_id=to, device_id_type=MESH
    ).start()


def wait_for(ref, sem):
    pltpu.make_async_copy(ref, ref, sem).wait()


def kernel(
    scale,
    src_hbm,
    det_hbm,
    probes_hbm,
    out,
    src_v,
    det_v,
    pr_v,
    pr_in,
    S,
    D,
    XS,
    XD,
    acc,
    tx,
    rx,
    zs,
    zr,
    mz,
    M,
    part,
    cv,
    ob,
    ld,
    pl_sem,
    ysend,
    yS,
    yD,
    pS,
    xsend,
    xD,
    whole,
    bsend,
    brecv,
    yB,
    cB,
    rsend,
    rrecv,
    zsend,
    zrecv,
    gsend,
    grecv,
    asend,
    arecv,
    fsend,
    frecv,
    ready,
):
    blk = lax.axis_index("blk")
    vox = lax.axis_index("vox")
    x, yh, c = blk // 4, (blk // 2) % 2, blk % 2
    z, yl = vox // 2, vox % 2
    y = yh * 2 + yl
    half = src_v.shape[1] // 2
    vc = half // NQ
    scope = jax.named_scope

    up, down = (y + 1) % NY, (y + 3) % NY
    xs = (x // 2) * 2 + 1 - x % 2
    xd = 3 - x
    me = x * 2 + c
    dev_up, dev_down = device(x, up, z, c), device(x, down, z, c)
    dev_xs, dev_xd = device(xs, y, z, c), device(xd, y, z, c)
    dev_c = device(x, y, z, 1 - c)

    def dev_z(d):
        return device(x, y, (z + NZ + d) % NZ, c)

    def signal(sem, to):
        pl.semaphore_signal(sem, inc=1, device_id=to, device_id_type=MESH)

    barrier = pltpu.get_barrier_semaphore()
    near = (dev_up, dev_down, dev_xs, dev_xd, dev_c, dev_z(1), dev_z(-1))
    for to in near:
        signal(barrier, to)

    h_up, h_down = up // 2, down // 2

    parts, turned = [], []
    for q in range(NQ):
        cuts = 2 if q in (0, NQ - 2) else 1
        for i in range(cuts):
            late = q == NQ - 1 or (q == NQ - 2 and i == 1)
            (turned if late else parts).append((q, i * vc // cuts, vc // cuts))
    last = len(parts)

    def columns(h, q, lo, wide):
        return pl.ds(pl.multiple_of(h * half + q * vc + lo, wide), wide)

    pltpu.make_async_copy(probes_hbm, pr_v, pl_sem).start()
    for q in (0, NQ - 2, *range(2, NQ - 2, 2)):
        for h in range(2):
            at = pl.ds(h * half + q * vc, 2 * vc)
            pltpu.make_async_copy(det_hbm.at[:, at], det_v.at[:, at], ld.at[q // 2, 0]).start()
            pltpu.make_async_copy(src_hbm.at[:, at], src_v.at[:, at], ld.at[q // 2, 1]).start()
    with scope("t_barrier"):
        pl.semaphore_wait(barrier, len(near))

    def spread_word(r):
        d = 2**r
        if r:
            pl.semaphore_wait(ready.at[r - 1], 2)
        if r < 3:
            signal(ready.at[r], dev_z(d))
            signal(ready.at[r], dev_z(-d))

    mine = pl.ds(pl.multiple_of(yh * 64, 64), 64)
    own, other = pl.ds(0, 128), pl.ds(128, 128)
    def swap(fields, here, i, sem, n):
        q, lo, wide = parts[n]
        if q % 2 == 0 and lo == 0 and q < NQ - 2:
            wait_for(D.at[q, pl.ds(0, 256)], ld.at[q // 2, i])
        to = (q, mine, pl.ds(lo, wide))
        send(fields.at[:, columns(h_up, q, lo, wide)], here.at[to], ysend.at[i], sem.at[n], dev_up)
        send(fields.at[:, columns(h_down, q, lo, wide)], here.at[to], ysend.at[i], sem.at[n], dev_down)

    for t in range(last):
        swap(det_v, D, 0, yD, t)
        swap(src_v, S, 1, yS, t)
        if t == 0:
            wait_for(pr_v, pl_sem)
            send(
                pr_v.at[:, pl.ds(pl.multiple_of(h_up * half, half), half)],
                pr_in,
                ysend.at[2],
                pS,
                dev_up,
            )
            spread_word(0)
        if t == 2:
            for i, (fields, there, to) in enumerate(((det_v, XD, dev_xd), (src_v, XS, dev_xs))):
                wait_for(D.at[0, pl.ds(0, 256)], ld.at[NQ // 2 - 1, i])
                for h in range(2):
                    at = pl.ds(h * half + turned[0][0] * vc + turned[0][1], there.shape[2])
                    send(fields.at[:, at], there.at[h], bsend.at[i], brecv.at[i], to)

    theirs = pl.ds(pl.multiple_of(128 + yh * 64, 64), 64)

    def swap_b():
        start = 0
        for n, (q, lo, wide) in enumerate(turned):
            for i, (fields, x_in, here) in enumerate(((det_v, XD, D), (src_v, XS, S))):
                at, x_at = pl.ds(lo, wide), pl.ds(start, wide)
                for h, to in ((h_up, dev_up), (h_down, dev_down)):
                    send(fields.at[:, columns(h, q, lo, wide)], here.at[q, mine, at], ysend.at[i], yB.at[i, n], to)
                if n == 0:
                    wait_for(x_in, brecv.at[i])
                for h, to in ((h_up, dev_up), (h_down, dev_down)):
                    send(x_in.at[h, :, x_at], here.at[q, theirs, at], bsend.at[2 + i], yB.at[i, n], to)
            start += wide

    def pass_b(n):
        q, at = turned[n][0], pl.ds(*turned[n][1:])
        wait_for(D.at[q, pl.ds(0, 256), at], yB.at[0, n])
        send(D.at[q, pl.ds(0, 256), at], D.at[q, pl.ds(256, 256), at], xsend.at[2], cB.at[n], dev_c)

    def pass_own(n):
        q, at = parts[n][0], pl.ds(*parts[n][1:])
        wait_for(D.at[q, own, at], yD.at[n])
        send(D.at[q, own, at], D.at[q, other, at], xsend.at[1], xD.at[n], dev_xd)
        send(D.at[q, own, at], D.at[q, pl.ds(256, 128), at], xsend.at[3], whole.at[n], dev_c)
        wait_for(S.at[q, own, at], yS.at[n])
        send(S.at[q, own, at], S.at[q, other, at], xsend.at[0], whole.at[n], dev_xs)

    def pass_other(n):
        q, at = parts[n][0], pl.ds(*parts[n][1:])
        wait_for(D.at[q, other, at], xD.at[n])
        send(D.at[q, other, at], D.at[q, pl.ds(384, 128), at], xsend.at[4], whole.at[n], dev_c)

    def measure(n):
        q, lo, wide = (parts + turned)[n]
        at = pl.ds(lo, wide)
        if n < last:
            wait_for(D.at[q, pl.ds(0, 384), at], whole.at[n])
        else:
            wait_for(D.at[q, pl.ds(256, 256), at], cB.at[n - last])
            wait_for(S.at[q, :, at], yB.at[1, n - last])
        fields = S[q, :, at].astype(F32)
        p = pr_in[:, q * vc + lo : q * vc + lo + wide].astype(F32)
        det = D[q, :, at]
        for k in range(2):
            weighted = (fields * p[k : k + 1]).astype(BF16)
            sums = lax.dot_general(weighted, det, (((1,), (1,)), ((), ())), preferred_element_type=F32)
            for g in range(4):
                piece = sums[:, g * 128 : (g + 1) * 128].reshape(4, 2, 32, 128)
                for h in range(2):
                    if n:
                        acc[k, 2 * g + h] += piece[:, h]
                    else:
                        acc[k, 2 * g + h] = piece[:, h]

    word = {3: 1, 6: 2}
    for t in range(last + 8):
        if t < last:
            with scope("g%02d_own" % t):
                pass_own(t)
        if t == 3:
            with scope("g%02d_b" % t):
                swap_b()
        if t in word:
            with scope("g%02d_word" % t):
                spread_word(word[t])
        if t - last in (0, 1):
            with scope("g%02d_b" % t):
                pass_b(t - last)
        if 0 <= t - 4 < last:
            with scope("g%02d_other" % t):
                pass_other(t - 4)
        if t == 6:
            wait_for(pr_in, pS)
        if 0 <= t - 6 < last + 2:
            with scope("g%02d_meas" % t):
                measure(t - 6)

    pairs = NZ // 2
    zp, zb = z // 2, z % 2
    s = 1 - 2 * zb
    away = (4, 3 * s, -3 * s, 2 * s, -2 * s, s, -s, 0)
    groups = [(zp + pairs + o) % pairs for o in away]
    turns = [(k, i) for k in range(2) for i in range(pairs)]
    for k, i in turns:
        for d in (2, 1, 3):
            to = (y + d) % NY
            tx[k, i, to] = acc[k, groups[i], to].astype(BF16)
            send(tx.at[k, i, to], rx.at[k, i, y], rsend, rrecv.at[k, i], device(x, to, z, c))
    spread_word(3)

    for k, i in turns:
        g = groups[i]
        with scope("r%d%d_y" % (k, i)):
            wait_for(rx.at[k, i, pl.ds(0, 3)], rrecv.at[k, i])
        total = acc[k, g, y]
        for d in (1, 2, 3):
            total += rx[k, i, (y + d) % NY].astype(F32)
        zs[k, i] = total.astype(BF16).reshape(2, 16, 128)
        for b in (0, 1) if i < pairs - 1 else (1 - zb,):
            send(zs.at[k, i, b], zr.at[k, z], zsend, zrecv.at[k], device(x, y, g * 2 + b, c))
    for k in range(2):
        zr[k, z] = zs[k, pairs - 1, zb]

    def back_along_z(k):
        with scope("r%d_z" % k):
            wait_for(zr.at[k, pl.ds(0, NZ - 1)], zrecv.at[k])
        total = zr[k, 0].astype(F32)
        for j in range(1, NZ):
            total += zr[k, j].astype(F32)
        mz[k] = total.astype(BF16)
        M[k, zp, y, zb] = mz[k]
        for step in range(NZ // 2, 0, -1):
            for to in (step, -step)[: 1 if step == NZ // 2 else 2]:
                send(mz.at[k], M.at[k, zp, y, zb], gsend, grecv.at[k, zp], dev_z(to))

    block, side = zp // 2, 2 * (zp % 2) - 1
    blocks = [(block + o) % 4 for o in (0, 4 + side, 4 - side, 2)]

    back = groups[::-1]

    def back_along_y(k):
        for i, g in enumerate(back):
            with scope("b%d%d_z" % (k, i)):
                wait_for(zr.at[k, pl.ds(0, 2 if i else 1)], grecv.at[k, g])
            off = (g // 2 - block + 4) % 4
            far = jnp.where((off == 0) | (off == (4 + side) % 4), 0, 1)
            for d in (2, 1, 3):
                send(M.at[k, g, y], M.at[k, g, y], asend, arecv.at[k, far], device(x, (y + d) % NY, z, c))

    def arrived(k, far):
        wait_for(M.at[k, pl.ds(0, 4), pl.ds(0, 3)], arecv.at[k, far])

    def contribution(k, q, lo):
        two = blocks[lo : lo + 2]
        lhs = jnp.concatenate([M[k, pl.ds(2 * g, 2)].reshape(256, 128) for g in two], axis=1)
        det = jnp.concatenate([D[q, pl.ds(pl.multiple_of(g * 128, 128), 128)] for g in two], axis=0)
        bp = jnp.dot(lhs, det, preferred_element_type=F32).reshape(2, 4, 32, vc)
        fields = S[q].astype(F32).reshape(4, 2, 32, vc)
        row = jnp.zeros((8, vc), F32)
        for h in range(2):
            row += jnp.sum((fields[:, h] * bp[h]).reshape(16, 8, vc), axis=0)
        return row

    def front(k):
        with scope("m%d_front" % k):
            arrived(k, 0)
            for q in range(NQ):
                part[k, q] = contribution(k, q, 0)

    def rest(k):
        with scope("m%d_y" % k):
            arrived(k, 1)
        per = NQ // NB
        with scope("m%d_rest" % k):
            for n in range(NB):
                rows = []
                for q in range(n * per, (n + 1) * per):
                    row = jnp.sum(part[k, q] + contribution(k, q, 2), axis=0, keepdims=True)
                    rows += [row[:, i * 128 : (i + 1) * 128] for i in range(vc // 128)]
                cv[k, n] = jnp.concatenate(rows, axis=0)
                for e in range(NX * NC):
                    for to in (up, down):
                        send(cv.at[k, n], ob.at[k, yh, me, n], fsend, frecv.at[k], device(e // 2, to, z, e % 2))

    def finish(k):
        with scope("f%d_recv" % k):
            wait_for(ob.at[k], frecv.at[k])
        wide = half // NB
        for h in range(2):
            for n in range(NB):
                total = ob[k, h, 0, n]
                for e in range(1, NX * NC):
                    total += ob[k, h, e, n]
                total = total * scale
                for i in range(wide // 128):
                    at = h * half + n * wide + i * 128
                    out[k : k + 1, at : at + 128] = total[i : i + 1]

    back_along_z(0)
    back_along_z(1)
    back_along_y(0)
    back_along_y(1)
    front(0)
    rest(0)
    front(1)
    rest(1)
    finish(0)
    finish(1)

    wait_for(det_v, ysend.at[0])
    wait_for(src_v, ysend.at[1])
    wait_for(pr_in, ysend.at[2])
    passed = det_v.at[:, pl.ds(0, 2 * sum(wide for _, _, wide in parts))]
    for i in (0, 1, 3, 4):
        wait_for(passed, xsend.at[i])
    wait_for(det_v.at[:, pl.ds(0, 4 * sum(wide for _, _, wide in turned))], xsend.at[2])
    for i in range(4):
        wait_for(XD, bsend.at[i])
    wait_for(tx.at[:, :, pl.ds(0, 3)], rsend)
    wait_for(zr.at[:, pl.ds(0, NZ - 1)], zsend)
    wait_for(zr.at[:, pl.ds(0, NZ - 1)], gsend)
    wait_for(M.at[:, :, pl.ds(0, 3)], asend)
    wait_for(ob, fsend)


def shards(src_fields, det_fields, probes):
    rows, voxels = src_fields.shape
    half = voxels // 2
    vc = half // NQ
    sources, detectors = rows * lax.axis_size("blk"), det_fields.shape[0] * lax.axis_size("blk")
    scale = 1.0 / (sources * detectors)
    hbm = pl.BlockSpec(memory_space=pl.ANY)
    given = [pltpu.with_memory_space_constraint(a, pltpu.HBM) for a in (src_fields, det_fields, probes)]
    return pl.pallas_call(
        functools.partial(kernel, scale),
        out_shape=jax.ShapeDtypeStruct((2, voxels), F32),
        in_specs=[hbm] * 3,
        out_specs=pl.BlockSpec(memory_space=pltpu.VMEM),
        scratch_shapes=[
            pltpu.VMEM((64, voxels), BF16),
            pltpu.VMEM((64, voxels), BF16),
            pltpu.VMEM((2, voxels), BF16),
            pltpu.VMEM((2, half), BF16),
            pltpu.VMEM((NQ, 256, vc), BF16),
            pltpu.VMEM((NQ, 512, vc), BF16),
            pltpu.VMEM((2, 64, 3 * vc // 2), BF16),
            pltpu.VMEM((2, 64, 3 * vc // 2), BF16),
            pltpu.VMEM((2, 8, 4, 32, 128), F32),
            pltpu.VMEM((2, 8, 4, 32, 128), BF16),
            pltpu.VMEM((2, 8, 4, 32, 128), BF16),
            pltpu.VMEM((2, 8, 2, 16, 128), BF16),
            pltpu.VMEM((2, NZ, 16, 128), BF16),
            pltpu.VMEM((2, 16, 128), BF16),
            pltpu.VMEM((2, 8, 4, 2, 16, 128), BF16),
            pltpu.VMEM((2, NQ, 8, vc), F32),
            pltpu.VMEM((2, NB, half // NB // 128, 128), F32),
            pltpu.VMEM((2, 2, NX * NC, NB, half // NB // 128, 128), F32),
            DMA((NQ // 2, 2)),
            DMA,
            DMA((3,)),
            DMA((NQ,)),
            DMA((NQ,)),
            DMA,
            DMA((5,)),
            DMA((NQ,)),
            DMA((NQ,)),
            DMA((4,)),
            DMA((2,)),
            DMA((2, 2)),
            DMA((2,)),
            DMA,
            DMA((2, 8)),
            DMA,
            DMA((2,)),
            DMA,
            DMA((2, 8)),
            DMA,
            DMA((2, 2)),
            DMA,
            DMA((2,)),
            pltpu.SemaphoreType.REGULAR((3,)),
        ],
        compiler_params=pltpu.CompilerParams(
            collective_id=0, has_side_effects=True, vmem_limit_bytes=50_000_000
        ),
        name="gauss_newton",
    )(*given)


def solution(mesh):
    return jax.shard_map(
        shards,
        mesh=mesh,
        in_specs=(P("blk", "vox"), P("blk", "vox"), P(None, "vox")),
        out_specs=P(None, "vox"),
        check_vma=False,
    )
```

```python
import functools

import jax
import jax.numpy as jnp
from jax import lax
from jax.experimental import pallas as pl
from jax.experimental.pallas import tpu as pltpu
from jax.sharding import PartitionSpec as P

MESH = pl.DeviceIdType.MESH
BF16 = jnp.bfloat16
F32 = jnp.float32
DMA = pltpu.SemaphoreType.DMA

NX, NY, NZ, NC = 4, 4, 16, 2
NQ = 8
NB = 2


def device(x, y, z, c):
    return (x * 4 + (y // 2) * 2 + c, z * 2 + y % 2)


def send(src, dst, send_sem, recv_sem, to):
    pltpu.make_async_remote_copy(
        src_ref=src, dst_ref=dst, send_sem=send_sem, recv_sem=recv_sem, device_id=to, device_id_type=MESH
    ).start()


def wait_for(ref, sem):
    pltpu.make_async_copy(ref, ref, sem).wait()


def kernel(
    scale,
    src_hbm,
    det_hbm,
    probes_hbm,
    out,
    src_v,
    det_v,
    pr_v,
    pr_in,
    S,
    D,
    XS,
    XD,
    acc,
    tx,
    rx,
    zs,
    zr,
    mz,
    M,
    part,
    cv,
    ob,
    ld,
    pl_sem,
    ysend,
    yS,
    yD,
    pS,
    xsend,
    xD,
    whole,
    bsend,
    brecv,
    yB,
    cB,
    rsend,
    rrecv,
    zsend,
    zrecv,
    gsend,
    grecv,
    asend,
    arecv,
    fsend,
    frecv,
    ready,
):
    blk = lax.axis_index("blk")
    vox = lax.axis_index("vox")
    x, yh, c = blk // 4, (blk // 2) % 2, blk % 2
    z, yl = vox // 2, vox % 2
    y = yh * 2 + yl
    half = src_v.shape[1] // 2
    vc = half // NQ
    scope = jax.named_scope

    up, down = (y + 1) % NY, (y + 3) % NY
    xs = (x // 2) * 2 + 1 - x % 2
    xd = 3 - x
    me = x * 2 + c
    dev_up, dev_down = device(x, up, z, c), device(x, down, z, c)
    dev_xs, dev_xd = device(xs, y, z, c), device(xd, y, z, c)
    dev_c = device(x, y, z, 1 - c)

    def dev_z(d):
        return device(x, y, (z + NZ + d) % NZ, c)

    def signal(sem, to):
        pl.semaphore_signal(sem, inc=1, device_id=to, device_id_type=MESH)

    barrier = pltpu.get_barrier_semaphore()
    near = (dev_up, dev_down, dev_xs, dev_xd, dev_c, dev_z(1), dev_z(-1))
    for to in near:
        signal(barrier, to)

    h_up, h_down = up // 2, down // 2

    parts, turned = [], []
    for q in range(NQ):
        cuts = 2 if q in (0, NQ - 2) else 1
        for i in range(cuts):
            late = q == NQ - 1 or (q == NQ - 2 and i == 1)
            (turned if late else parts).append((q, i * vc // cuts, vc // cuts))
    last = len(parts)

    def columns(h, q, lo, wide):
        return pl.ds(pl.multiple_of(h * half + q * vc + lo, wide), wide)

    pltpu.make_async_copy(probes_hbm, pr_v, pl_sem).start()
    for q in (0, NQ - 2, *range(2, NQ - 2, 2)):
        for h in range(2):
            at = pl.ds(h * half + q * vc, 2 * vc)
            pltpu.make_async_copy(det_hbm.at[:, at], det_v.at[:, at], ld.at[q // 2, 0]).start()
            pltpu.make_async_copy(src_hbm.at[:, at], src_v.at[:, at], ld.at[q // 2, 1]).start()
    with scope("t_barrier"):
        pl.semaphore_wait(barrier, len(near))

    def spread_word(r):
        d = 2**r
        if r:
            pl.semaphore_wait(ready.at[r - 1], 2)
        if r < 3:
            signal(ready.at[r], dev_z(d))
            signal(ready.at[r], dev_z(-d))

    mine = pl.ds(pl.multiple_of(yh * 64, 64), 64)
    own, other = pl.ds(0, 128), pl.ds(128, 128)
    def swap(fields, here, i, sem, n):
        q, lo, wide = parts[n]
        if q % 2 == 0 and lo == 0 and q < NQ - 2:
            wait_for(D.at[q, pl.ds(0, 256)], ld.at[q // 2, i])
        to = (q, mine, pl.ds(lo, wide))
        send(fields.at[:, columns(h_up, q, lo, wide)], here.at[to], ysend.at[i], sem.at[n], dev_up)
        send(fields.at[:, columns(h_down, q, lo, wide)], here.at[to], ysend.at[i], sem.at[n], dev_down)

    for t in range(last):
        swap(det_v, D, 0, yD, t)
        swap(src_v, S, 1, yS, t)
        if t == 0:
            wait_for(pr_v, pl_sem)
            send(
                pr_v.at[:, pl.ds(pl.multiple_of(h_up * half, half), half)],
                pr_in,
                ysend.at[2],
                pS,
                dev_up,
            )
            spread_word(0)
        if t == 2:
            for i, (fields, there, to) in enumerate(((det_v, XD, dev_xd), (src_v, XS, dev_xs))):
                wait_for(D.at[0, pl.ds(0, 256)], ld.at[NQ // 2 - 1, i])
                for h in range(2):
                    at = pl.ds(h * half + turned[0][0] * vc + turned[0][1], there.shape[2])
                    send(fields.at[:, at], there.at[h], bsend.at[i], brecv.at[i], to)

    theirs = pl.ds(pl.multiple_of(128 + yh * 64, 64), 64)

    def swap_b():
        start = 0
        for n, (q, lo, wide) in enumerate(turned):
            for i, (fields, x_in, here) in enumerate(((det_v, XD, D), (src_v, XS, S))):
                at, x_at = pl.ds(lo, wide), pl.ds(start, wide)
                for h, to in ((h_up, dev_up), (h_down, dev_down)):
                    send(fields.at[:, columns(h, q, lo, wide)], here.at[q, mine, at], ysend.at[i], yB.at[i, n], to)
                if n == 0:
                    wait_for(x_in, brecv.at[i])
                for h, to in ((h_up, dev_up), (h_down, dev_down)):
                    send(x_in.at[h, :, x_at], here.at[q, theirs, at], bsend.at[2 + i], yB.at[i, n], to)
            start += wide

    def pass_b(n):
        q, at = turned[n][0], pl.ds(*turned[n][1:])
        wait_for(D.at[q, pl.ds(0, 256), at], yB.at[0, n])
        send(D.at[q, pl.ds(0, 256), at], D.at[q, pl.ds(256, 256), at], xsend.at[2], cB.at[n], dev_c)

    def pass_own(n):
        q, at = parts[n][0], pl.ds(*parts[n][1:])
        wait_for(D.at[q, own, at], yD.at[n])
        send(D.at[q, own, at], D.at[q, other, at], xsend.at[1], xD.at[n], dev_xd)
        send(D.at[q, own, at], D.at[q, pl.ds(256, 128), at], xsend.at[3], whole.at[n], dev_c)
        wait_for(S.at[q, own, at], yS.at[n])
        send(S.at[q, own, at], S.at[q, other, at], xsend.at[0], whole.at[n], dev_xs)

    def pass_other(n):
        q, at = parts[n][0], pl.ds(*parts[n][1:])
        wait_for(D.at[q, other, at], xD.at[n])
        send(D.at[q, other, at], D.at[q, pl.ds(384, 128), at], xsend.at[4], whole.at[n], dev_c)

    def measure(n):
        q, lo, wide = (parts + turned)[n]
        at = pl.ds(lo, wide)
        if n < last:
            wait_for(D.at[q, pl.ds(0, 384), at], whole.at[n])
        else:
            wait_for(D.at[q, pl.ds(256, 256), at], cB.at[n - last])
            wait_for(S.at[q, :, at], yB.at[1, n - last])
        fields = S[q, :, at].astype(F32)
        p = pr_in[:, q * vc + lo : q * vc + lo + wide].astype(F32)
        det = D[q, :, at]
        for k in range(2):
            weighted = (fields * p[k : k + 1]).astype(BF16)
            sums = lax.dot_general(weighted, det, (((1,), (1,)), ((), ())), preferred_element_type=F32)
            for g in range(4):
                piece = sums[:, g * 128 : (g + 1) * 128].reshape(4, 2, 32, 128)
                for h in range(2):
                    if n:
                        acc[k, 2 * g + h] += piece[:, h]
                    else:
                        acc[k, 2 * g + h] = piece[:, h]

    steps = []
    for t in range(last):
        steps.append((pass_own, t))
        if t == 3:
            steps.append((spread_word, 1))
        if t == 6:
            steps.append((spread_word, 2))
        if t >= 3:
            steps.append((pass_other, t - 3))
        if t >= 5:
            steps.append((measure, t - 5))
    n = last
    steps += [(pass_other, n - 3), (pass_b, 0), (measure, n - 5), (measure, n - 4), (pass_other, n - 2)]
    steps += [(measure, n - 3), (measure, n), (pass_other, n - 1), (pass_b, 1)]
    steps += [(measure, n - 2), (measure, n - 1), (measure, n + 1)]
    for t, (step, n) in enumerate(steps):
        if step is measure and n == 0:
            wait_for(pr_in, pS)
        with scope("g%02d_%s%d" % (t, step.__name__, n)):
            step(n)
        if step is pass_own and n == 3:
            swap_b()

    pairs = NZ // 2
    zp, zb = z // 2, z % 2
    s = 1 - 2 * zb
    away = (4, 3 * s, -3 * s, 2 * s, -2 * s, s, -s, 0)
    groups = [(zp + pairs + o) % pairs for o in away]
    turns = [(k, i) for k in range(2) for i in range(pairs)]
    for k, i in turns:
        for d in (2, 1, 3):
            to = (y + d) % NY
            tx[k, i, to] = acc[k, groups[i], to].astype(BF16)
            send(tx.at[k, i, to], rx.at[k, i, y], rsend, rrecv.at[k, i], device(x, to, z, c))
    spread_word(3)

    for k, i in turns:
        g = groups[i]
        with scope("r%d%d_y" % (k, i)):
            wait_for(rx.at[k, i, pl.ds(0, 3)], rrecv.at[k, i])
        total = acc[k, g, y]
        for d in (1, 2, 3):
            total += rx[k, i, (y + d) % NY].astype(F32)
        zs[k, i] = total.astype(BF16).reshape(2, 16, 128)
        for b in (0, 1) if i < pairs - 1 else (1 - zb,):
            send(zs.at[k, i, b], zr.at[k, z], zsend, zrecv.at[k], device(x, y, g * 2 + b, c))
    for k in range(2):
        zr[k, z] = zs[k, pairs - 1, zb]

    def back_along_z(k):
        with scope("r%d_z" % k):
            wait_for(zr.at[k, pl.ds(0, NZ - 1)], zrecv.at[k])
        total = zr[k, 0].astype(F32)
        for j in range(1, NZ):
            total += zr[k, j].astype(F32)
        mz[k] = total.astype(BF16)
        M[k, zp, y, zb] = mz[k]
        for step in range(NZ // 2, 0, -1):
            for to in (step, -step)[: 1 if step == NZ // 2 else 2]:
                send(mz.at[k], M.at[k, zp, y, zb], gsend, grecv.at[k, zp], dev_z(to))

    block, side = zp // 2, 2 * (zp % 2) - 1
    blocks = [(block + o) % 4 for o in (0, 4 + side, 4 - side, 2)]

    back = groups[::-1]

    def back_along_y(k):
        for i, g in enumerate(back):
            with scope("b%d%d_z" % (k, i)):
                wait_for(zr.at[k, pl.ds(0, 2 if i else 1)], grecv.at[k, g])
            off = (g // 2 - block + 4) % 4
            far = jnp.where((off == 0) | (off == (4 + side) % 4), 0, 1)
            for d in (2, 1, 3):
                send(M.at[k, g, y], M.at[k, g, y], asend, arecv.at[k, far], device(x, (y + d) % NY, z, c))

    def arrived(k, far):
        wait_for(M.at[k, pl.ds(0, 4), pl.ds(0, 3)], arecv.at[k, far])

    def contribution(k, q, lo):
        two = blocks[lo : lo + 2]
        lhs = jnp.concatenate([M[k, pl.ds(2 * g, 2)].reshape(256, 128) for g in two], axis=1)
        det = jnp.concatenate([D[q, pl.ds(pl.multiple_of(g * 128, 128), 128)] for g in two], axis=0)
        bp = jnp.dot(lhs, det, preferred_element_type=F32).reshape(2, 4, 32, vc)
        fields = S[q].astype(F32).reshape(4, 2, 32, vc)
        row = jnp.zeros((8, vc), F32)
        for h in range(2):
            row += jnp.sum((fields[:, h] * bp[h]).reshape(16, 8, vc), axis=0)
        return row

    def front(k):
        with scope("m%d_front" % k):
            arrived(k, 0)
            for q in range(NQ):
                part[k, q] = contribution(k, q, 0)

    def rest(k):
        with scope("m%d_y" % k):
            arrived(k, 1)
        per = NQ // NB
        with scope("m%d_rest" % k):
            for n in range(NB):
                rows = []
                for q in range(n * per, (n + 1) * per):
                    row = jnp.sum(part[k, q] + contribution(k, q, 2), axis=0, keepdims=True)
                    rows += [row[:, i * 128 : (i + 1) * 128] for i in range(vc // 128)]
                cv[k, n] = jnp.concatenate(rows, axis=0)
                for e in range(NX * NC):
                    for to in (up, down):
                        send(cv.at[k, n], ob.at[k, yh, me, n], fsend, frecv.at[k], device(e // 2, to, z, e % 2))

    def finish(k):
        with scope("f%d_recv" % k):
            wait_for(ob.at[k], frecv.at[k])
        wide = half // NB
        for h in range(2):
            for n in range(NB):
                total = ob[k, h, 0, n]
                for e in range(1, NX * NC):
                    total += ob[k, h, e, n]
                total = total * scale
                for i in range(wide // 128):
                    at = h * half + n * wide + i * 128
                    out[k : k + 1, at : at + 128] = total[i : i + 1]

    back_along_z(0)
    back_along_z(1)
    back_along_y(0)
    back_along_y(1)
    front(0)
    rest(0)
    front(1)
    rest(1)
    finish(0)
    finish(1)

    wait_for(det_v, ysend.at[0])
    wait_for(src_v, ysend.at[1])
    wait_for(pr_in, ysend.at[2])
    passed = det_v.at[:, pl.ds(0, 2 * sum(wide for _, _, wide in parts))]
    for i in (0, 1, 3, 4):
        wait_for(passed, xsend.at[i])
    wait_for(det_v.at[:, pl.ds(0, 4 * sum(wide for _, _, wide in turned))], xsend.at[2])
    for i in range(4):
        wait_for(XD, bsend.at[i])
    wait_for(tx.at[:, :, pl.ds(0, 3)], rsend)
    wait_for(zr.at[:, pl.ds(0, NZ - 1)], zsend)
    wait_for(zr.at[:, pl.ds(0, NZ - 1)], gsend)
    wait_for(M.at[:, :, pl.ds(0, 3)], asend)
    wait_for(ob, fsend)


def shards(src_fields, det_fields, probes):
    rows, voxels = src_fields.shape
    half = voxels // 2
    vc = half // NQ
    sources, detectors = rows * lax.axis_size("blk"), det_fields.shape[0] * lax.axis_size("blk")
    scale = 1.0 / (sources * detectors)
    hbm = pl.BlockSpec(memory_space=pl.ANY)
    given = [pltpu.with_memory_space_constraint(a, pltpu.HBM) for a in (src_fields, det_fields, probes)]
    return pl.pallas_call(
        functools.partial(kernel, scale),
        out_shape=jax.ShapeDtypeStruct((2, voxels), F32),
        in_specs=[hbm] * 3,
        out_specs=pl.BlockSpec(memory_space=pltpu.VMEM),
        scratch_shapes=[
            pltpu.VMEM((64, voxels), BF16),
            pltpu.VMEM((64, voxels), BF16),
            pltpu.VMEM((2, voxels), BF16),
            pltpu.VMEM((2, half), BF16),
            pltpu.VMEM((NQ, 256, vc), BF16),
            pltpu.VMEM((NQ, 512, vc), BF16),
            pltpu.VMEM((2, 64, 3 * vc // 2), BF16),
            pltpu.VMEM((2, 64, 3 * vc // 2), BF16),
            pltpu.VMEM((2, 8, 4, 32, 128), F32),
            pltpu.VMEM((2, 8, 4, 32, 128), BF16),
            pltpu.VMEM((2, 8, 4, 32, 128), BF16),
            pltpu.VMEM((2, 8, 2, 16, 128), BF16),
            pltpu.VMEM((2, NZ, 16, 128), BF16),
            pltpu.VMEM((2, 16, 128), BF16),
            pltpu.VMEM((2, 8, 4, 2, 16, 128), BF16),
            pltpu.VMEM((2, NQ, 8, vc), F32),
            pltpu.VMEM((2, NB, half // NB // 128, 128), F32),
            pltpu.VMEM((2, 2, NX * NC, NB, half // NB // 128, 128), F32),
            DMA((NQ // 2, 2)),
            DMA,
            DMA((3,)),
            DMA((NQ,)),
            DMA((NQ,)),
            DMA,
            DMA((5,)),
            DMA((NQ,)),
            DMA((NQ,)),
            DMA((4,)),
            DMA((2,)),
            DMA((2, 2)),
            DMA((2,)),
            DMA,
            DMA((2, 8)),
            DMA,
            DMA((2,)),
            DMA,
            DMA((2, 8)),
            DMA,
            DMA((2, 2)),
            DMA,
            DMA((2,)),
            pltpu.SemaphoreType.REGULAR((3,)),
        ],
        compiler_params=pltpu.CompilerParams(
            collective_id=0, has_side_effects=True, vmem_limit_bytes=50_000_000
        ),
        name="gauss_newton",
    )(*given)


def solution(mesh):
    return jax.shard_map(
        shards,
        mesh=mesh,
        in_specs=(P("blk", "vox"), P("blk", "vox"), P(None, "vox")),
        out_specs=P(None, "vox"),
        check_vma=False,
    )
```

```python
import functools

import jax
import jax.numpy as jnp
from jax import lax
from jax.experimental import pallas as pl
from jax.experimental.pallas import tpu as pltpu
from jax.sharding import PartitionSpec as P

MESH = pl.DeviceIdType.MESH
BF16 = jnp.bfloat16
F32 = jnp.float32
DMA = pltpu.SemaphoreType.DMA

NX, NY, NZ, NC = 4, 4, 16, 2
NQ = 8
NB = 2


def device(x, y, z, c):
    return (x * 4 + (y // 2) * 2 + c, z * 2 + y % 2)


def send(src, dst, send_sem, recv_sem, to):
    pltpu.make_async_remote_copy(
        src_ref=src, dst_ref=dst, send_sem=send_sem, recv_sem=recv_sem, device_id=to, device_id_type=MESH
    ).start()


def wait_for(ref, sem):
    pltpu.make_async_copy(ref, ref, sem).wait()


def kernel(
    scale,
    src_hbm,
    det_hbm,
    probes_hbm,
    out,
    src_v,
    det_v,
    pr_v,
    pr_in,
    S,
    D,
    XS,
    XD,
    acc,
    tx,
    rx,
    zs,
    zr,
    mz,
    M,
    part,
    cv,
    ob,
    ld,
    pl_sem,
    ysend,
    yS,
    yD,
    pS,
    xsend,
    xD,
    whole,
    bsend,
    brecv,
    yB,
    cB,
    rsend,
    rrecv,
    zsend,
    zrecv,
    gsend,
    grecv,
    asend,
    arecv,
    fsend,
    frecv,
    ready,
):
    blk = lax.axis_index("blk")
    vox = lax.axis_index("vox")
    x, yh, c = blk // 4, (blk // 2) % 2, blk % 2
    z, yl = vox // 2, vox % 2
    y = yh * 2 + yl
    half = src_v.shape[1] // 2
    vc = half // NQ
    scope = jax.named_scope

    up, down = (y + 1) % NY, (y + 3) % NY
    xd = (x // 2) * 2 + 1 - x % 2
    xs = 3 - x
    me = x * 2 + c
    dev_up, dev_down = device(x, up, z, c), device(x, down, z, c)
    dev_xs, dev_xd = device(xs, y, z, c), device(xd, y, z, c)
    dev_c = device(x, y, z, 1 - c)

    def dev_z(d):
        return device(x, y, (z + NZ + d) % NZ, c)

    def signal(sem, to):
        pl.semaphore_signal(sem, inc=1, device_id=to, device_id_type=MESH)

    barrier = pltpu.get_barrier_semaphore()
    near = (dev_up, dev_down, dev_xs, dev_xd, dev_c, dev_z(1), dev_z(-1))
    for to in near:
        signal(barrier, to)

    h_up, h_down = up // 2, down // 2

    parts, turned = [], []
    for q in range(NQ):
        cuts = 2 if q in (0, NQ - 2) else 1
        for i in range(cuts):
            late = q == NQ - 1 or (q == NQ - 2 and i == 1)
            (turned if late else parts).append((q, i * vc // cuts, vc // cuts))
    last = len(parts)

    def columns(h, q, lo, wide):
        return pl.ds(pl.multiple_of(h * half + q * vc + lo, wide), wide)

    pltpu.make_async_copy(probes_hbm, pr_v, pl_sem).start()
    for q in (0, NQ - 2, *range(2, NQ - 2, 2)):
        for h in range(2):
            at = pl.ds(h * half + q * vc, 2 * vc)
            pltpu.make_async_copy(det_hbm.at[:, at], det_v.at[:, at], ld.at[q // 2, 0]).start()
            pltpu.make_async_copy(src_hbm.at[:, at], src_v.at[:, at], ld.at[q // 2, 1]).start()
    with scope("t_barrier"):
        pl.semaphore_wait(barrier, len(near))

    def spread_word(r):
        d = 2**r
        if r:
            pl.semaphore_wait(ready.at[r - 1], 2)
        if r < 3:
            signal(ready.at[r], dev_z(d))
            signal(ready.at[r], dev_z(-d))

    mine = pl.ds(pl.multiple_of(yh * 64, 64), 64)
    own, other = pl.ds(0, 128), pl.ds(128, 128)
    def swap(fields, here, i, sem, n):
        q, lo, wide = parts[n]
        if q % 2 == 0 and lo == 0 and q < NQ - 2:
            wait_for(D.at[q, pl.ds(0, 256)], ld.at[q // 2, i])
        to = (q, mine, pl.ds(lo, wide))
        send(fields.at[:, columns(h_up, q, lo, wide)], here.at[to], ysend.at[i], sem.at[n], dev_up)
        send(fields.at[:, columns(h_down, q, lo, wide)], here.at[to], ysend.at[i], sem.at[n], dev_down)

    for t in range(last):
        swap(det_v, D, 0, yD, t)
        swap(src_v, S, 1, yS, t)
        if t == 0:
            wait_for(pr_v, pl_sem)
            send(
                pr_v.at[:, pl.ds(pl.multiple_of(h_up * half, half), half)],
                pr_in,
                ysend.at[2],
                pS,
                dev_up,
            )
            spread_word(0)
        if t == 2:
            for i, (fields, there, to) in enumerate(((det_v, XD, dev_xd), (src_v, XS, dev_xs))):
                wait_for(D.at[0, pl.ds(0, 256)], ld.at[NQ // 2 - 1, i])
                for h in range(2):
                    at = pl.ds(h * half + turned[0][0] * vc + turned[0][1], there.shape[2])
                    send(fields.at[:, at], there.at[h], bsend.at[i], brecv.at[i], to)

    theirs = pl.ds(pl.multiple_of(128 + yh * 64, 64), 64)

    def swap_b():
        start = 0
        for n, (q, lo, wide) in enumerate(turned):
            for i, (fields, x_in, here) in enumerate(((det_v, XD, D), (src_v, XS, S))):
                at, x_at = pl.ds(lo, wide), pl.ds(start, wide)
                for h, to in ((h_up, dev_up), (h_down, dev_down)):
                    send(fields.at[:, columns(h, q, lo, wide)], here.at[q, mine, at], ysend.at[i], yB.at[i, n], to)
                if n == 0:
                    wait_for(x_in, brecv.at[i])
                for h, to in ((h_up, dev_up), (h_down, dev_down)):
                    send(x_in.at[h, :, x_at], here.at[q, theirs, at], bsend.at[2 + i], yB.at[i, n], to)
            start += wide

    def pass_b(n):
        q, at = turned[n][0], pl.ds(*turned[n][1:])
        wait_for(D.at[q, pl.ds(0, 256), at], yB.at[0, n])
        send(D.at[q, pl.ds(0, 256), at], D.at[q, pl.ds(256, 256), at], xsend.at[2], cB.at[n], dev_c)

    def pass_own(n):
        q, at = parts[n][0], pl.ds(*parts[n][1:])
        wait_for(D.at[q, own, at], yD.at[n])
        send(D.at[q, own, at], D.at[q, other, at], xsend.at[1], xD.at[n], dev_xd)
        send(D.at[q, own, at], D.at[q, pl.ds(256, 128), at], xsend.at[3], whole.at[n], dev_c)
        wait_for(S.at[q, own, at], yS.at[n])
        send(S.at[q, own, at], S.at[q, other, at], xsend.at[0], whole.at[n], dev_xs)

    def pass_other(n):
        q, at = parts[n][0], pl.ds(*parts[n][1:])
        wait_for(D.at[q, other, at], xD.at[n])
        send(D.at[q, other, at], D.at[q, pl.ds(384, 128), at], xsend.at[4], whole.at[n], dev_c)

    def measure(n):
        q, lo, wide = (parts + turned)[n]
        at = pl.ds(lo, wide)
        if n < last:
            wait_for(D.at[q, pl.ds(0, 384), at], whole.at[n])
        else:
            wait_for(D.at[q, pl.ds(256, 256), at], cB.at[n - last])
            wait_for(S.at[q, :, at], yB.at[1, n - last])
        fields = S[q, :, at].astype(F32)
        p = pr_in[:, q * vc + lo : q * vc + lo + wide].astype(F32)
        det = D[q, :, at]
        for k in range(2):
            weighted = (fields * p[k : k + 1]).astype(BF16)
            sums = lax.dot_general(weighted, det, (((1,), (1,)), ((), ())), preferred_element_type=F32)
            for g in range(4):
                piece = sums[:, g * 128 : (g + 1) * 128].reshape(4, 2, 32, 128)
                for h in range(2):
                    if n:
                        acc[k, 2 * g + h] += piece[:, h]
                    else:
                        acc[k, 2 * g + h] = piece[:, h]

    steps = []
    for t in range(last):
        steps.append((pass_own, t))
        if t == 3:
            steps.append((spread_word, 1))
        if t == 6:
            steps.append((spread_word, 2))
        if t >= 3:
            steps.append((pass_other, t - 3))
        if t >= 5:
            steps.append((measure, t - 5))
    n = last
    steps += [(pass_other, n - 3), (pass_b, 0), (measure, n - 5), (measure, n - 4), (pass_other, n - 2)]
    steps += [(measure, n - 3), (measure, n), (pass_other, n - 1), (pass_b, 1)]
    steps += [(measure, n - 2), (measure, n - 1), (measure, n + 1)]
    for t, (step, n) in enumerate(steps):
        if step is measure and n == 0:
            wait_for(pr_in, pS)
        with scope("g%02d_%s%d" % (t, step.__name__, n)):
            step(n)
        if step is pass_own and n == 3:
            swap_b()

    pairs = NZ // 2
    zp, zb = z // 2, z % 2
    s = 1 - 2 * zb
    away = (4, 3 * s, -3 * s, 2 * s, -2 * s, s, -s, 0)
    groups = [(zp + pairs + o) % pairs for o in away]
    turns = [(k, i) for k in range(2) for i in range(pairs)]
    for k, i in turns:
        for d in (2, 1, 3):
            to = (y + d) % NY
            tx[k, i, to] = acc[k, groups[i], to].astype(BF16)
            send(tx.at[k, i, to], rx.at[k, i, y], rsend, rrecv.at[k, i], device(x, to, z, c))
    spread_word(3)

    for k, i in turns:
        g = groups[i]
        with scope("r%d%d_y" % (k, i)):
            wait_for(rx.at[k, i, pl.ds(0, 3)], rrecv.at[k, i])
        total = acc[k, g, y]
        for d in (1, 2, 3):
            total += rx[k, i, (y + d) % NY].astype(F32)
        zs[k, i] = total.astype(BF16).reshape(2, 16, 128)
        for b in (0, 1) if i < pairs - 1 else (1 - zb,):
            send(zs.at[k, i, b], zr.at[k, z], zsend, zrecv.at[k], device(x, y, g * 2 + b, c))
    for k in range(2):
        zr[k, z] = zs[k, pairs - 1, zb]

    def back_along_z(k):
        with scope("r%d_z" % k):
            wait_for(zr.at[k, pl.ds(0, NZ - 1)], zrecv.at[k])
        total = zr[k, 0].astype(F32)
        for j in range(1, NZ):
            total += zr[k, j].astype(F32)
        mz[k] = total.astype(BF16)
        M[k, zp, y, zb] = mz[k]
        for step in range(NZ // 2, 0, -1):
            for to in (step, -step)[: 1 if step == NZ // 2 else 2]:
                send(mz.at[k], M.at[k, zp, y, zb], gsend, grecv.at[k, zp], dev_z(to))

    block, side = zp // 2, 2 * (zp % 2) - 1
    blocks = [(block + o) % 4 for o in (0, 4 + side, 4 - side, 2)]

    back = groups[::-1]

    def back_along_y(k):
        for i, g in enumerate(back):
            with scope("b%d%d_z" % (k, i)):
                wait_for(zr.at[k, pl.ds(0, 2 if i else 1)], grecv.at[k, g])
            off = (g // 2 - block + 4) % 4
            far = jnp.where((off == 0) | (off == (4 + side) % 4), 0, 1)
            for d in (2, 1, 3):
                send(M.at[k, g, y], M.at[k, g, y], asend, arecv.at[k, far], device(x, (y + d) % NY, z, c))

    def arrived(k, far):
        wait_for(M.at[k, pl.ds(0, 4), pl.ds(0, 3)], arecv.at[k, far])

    def contribution(k, q, lo):
        two = blocks[lo : lo + 2]
        lhs = jnp.concatenate([M[k, pl.ds(2 * g, 2)].reshape(256, 128) for g in two], axis=1)
        det = jnp.concatenate([D[q, pl.ds(pl.multiple_of(g * 128, 128), 128)] for g in two], axis=0)
        bp = jnp.dot(lhs, det, preferred_element_type=F32).reshape(2, 4, 32, vc)
        fields = S[q].astype(F32).reshape(4, 2, 32, vc)
        row = jnp.zeros((8, vc), F32)
        for h in range(2):
            row += jnp.sum((fields[:, h] * bp[h]).reshape(16, 8, vc), axis=0)
        return row

    def front(k):
        with scope("m%d_front" % k):
            arrived(k, 0)
            for q in range(NQ):
                part[k, q] = contribution(k, q, 0)

    def rest(k):
        with scope("m%d_y" % k):
            arrived(k, 1)
        per = NQ // NB
        with scope("m%d_rest" % k):
            for n in range(NB):
                rows = []
                for q in range(n * per, (n + 1) * per):
                    row = jnp.sum(part[k, q] + contribution(k, q, 2), axis=0, keepdims=True)
                    rows += [row[:, i * 128 : (i + 1) * 128] for i in range(vc // 128)]
                cv[k, n] = jnp.concatenate(rows, axis=0)
                for e in range(NX * NC):
                    for to in (up, down):
                        send(cv.at[k, n], ob.at[k, yh, me, n], fsend, frecv.at[k], device(e // 2, to, z, e % 2))

    def finish(k):
        with scope("f%d_recv" % k):
            wait_for(ob.at[k], frecv.at[k])
        wide = half // NB
        for h in range(2):
            for n in range(NB):
                total = ob[k, h, 0, n]
                for e in range(1, NX * NC):
                    total += ob[k, h, e, n]
                total = total * scale
                for i in range(wide // 128):
                    at = h * half + n * wide + i * 128
                    out[k : k + 1, at : at + 128] = total[i : i + 1]

    back_along_z(0)
    back_along_z(1)
    back_along_y(0)
    back_along_y(1)
    front(0)
    rest(0)
    front(1)
    rest(1)
    finish(0)

    wait_for(det_v, ysend.at[0])
    wait_for(src_v, ysend.at[1])
    wait_for(pr_in, ysend.at[2])
    passed = det_v.at[:, pl.ds(0, 2 * sum(wide for _, _, wide in parts))]
    for i in (0, 1, 3, 4):
        wait_for(passed, xsend.at[i])
    wait_for(det_v.at[:, pl.ds(0, 4 * sum(wide for _, _, wide in turned))], xsend.at[2])
    for i in range(4):
        wait_for(XD, bsend.at[i])
    wait_for(tx.at[:, :, pl.ds(0, 3)], rsend)
    wait_for(zr.at[:, pl.ds(0, NZ - 1)], zsend)
    wait_for(zr.at[:, pl.ds(0, NZ - 1)], gsend)
    wait_for(M.at[:, :, pl.ds(0, 3)], asend)
    wait_for(ob, fsend)
    finish(1)


def shards(src_fields, det_fields, probes):
    rows, voxels = src_fields.shape
    half = voxels // 2
    vc = half // NQ
    sources, detectors = rows * lax.axis_size("blk"), det_fields.shape[0] * lax.axis_size("blk")
    scale = 1.0 / (sources * detectors)
    hbm = pl.BlockSpec(memory_space=pl.ANY)
    given = [pltpu.with_memory_space_constraint(a, pltpu.HBM) for a in (src_fields, det_fields, probes)]
    return pl.pallas_call(
        functools.partial(kernel, scale),
        out_shape=jax.ShapeDtypeStruct((2, voxels), F32),
        in_specs=[hbm] * 3,
        out_specs=pl.BlockSpec(memory_space=pltpu.VMEM),
        scratch_shapes=[
            pltpu.VMEM((64, voxels), BF16),
            pltpu.VMEM((64, voxels), BF16),
            pltpu.VMEM((2, voxels), BF16),
            pltpu.VMEM((2, half), BF16),
            pltpu.VMEM((NQ, 256, vc), BF16),
            pltpu.VMEM((NQ, 512, vc), BF16),
            pltpu.VMEM((2, 64, 3 * vc // 2), BF16),
            pltpu.VMEM((2, 64, 3 * vc // 2), BF16),
            pltpu.VMEM((2, 8, 4, 32, 128), F32),
            pltpu.VMEM((2, 8, 4, 32, 128), BF16),
            pltpu.VMEM((2, 8, 4, 32, 128), BF16),
            pltpu.VMEM((2, 8, 2, 16, 128), BF16),
            pltpu.VMEM((2, NZ, 16, 128), BF16),
            pltpu.VMEM((2, 16, 128), BF16),
            pltpu.VMEM((2, 8, 4, 2, 16, 128), BF16),
            pltpu.VMEM((2, NQ, 8, vc), F32),
            pltpu.VMEM((2, NB, half // NB // 128, 128), F32),
            pltpu.VMEM((2, 2, NX * NC, NB, half // NB // 128, 128), F32),
            DMA((NQ // 2, 2)),
            DMA,
            DMA((3,)),
            DMA((NQ,)),
            DMA((NQ,)),
            DMA,
            DMA((5,)),
            DMA((NQ,)),
            DMA((NQ,)),
            DMA((4,)),
            DMA((2,)),
            DMA((2, 2)),
            DMA((2,)),
            DMA,
            DMA((2, 8)),
            DMA,
            DMA((2,)),
            DMA,
            DMA((2, 8)),
            DMA,
            DMA((2, 2)),
            DMA,
            DMA((2,)),
            pltpu.SemaphoreType.REGULAR((3,)),
        ],
        compiler_params=pltpu.CompilerParams(
            collective_id=0, has_side_effects=True, vmem_limit_bytes=50_000_000
        ),
        name="gauss_newton",
    )(*given)


def solution(mesh):
    return jax.shard_map(
        shards,
        mesh=mesh,
        in_specs=(P("blk", "vox"), P("blk", "vox"), P(None, "vox")),
        out_specs=P(None, "vox"),
        check_vma=False,
    )
```

```python
import functools

import jax
import jax.numpy as jnp
from jax import lax
from jax.experimental import pallas as pl
from jax.experimental.pallas import tpu as pltpu
from jax.sharding import PartitionSpec as P

MESH = pl.DeviceIdType.MESH
BF16 = jnp.bfloat16
F32 = jnp.float32
DMA = pltpu.SemaphoreType.DMA

NX, NY, NZ, NC = 4, 4, 16, 2
NQ = 8
NB = 2


def device(x, y, z, c):
    return (x * 4 + (y // 2) * 2 + c, z * 2 + y % 2)


def send(src, dst, send_sem, recv_sem, to):
    pltpu.make_async_remote_copy(
        src_ref=src, dst_ref=dst, send_sem=send_sem, recv_sem=recv_sem, device_id=to, device_id_type=MESH
    ).start()


def wait_for(ref, sem):
    pltpu.make_async_copy(ref, ref, sem).wait()


def kernel(
    scale,
    src_hbm,
    det_hbm,
    probes_hbm,
    out,
    src_v,
    det_v,
    pr_v,
    pr_in,
    S,
    D,
    XS,
    XD,
    acc,
    tx,
    rx,
    zs,
    zr,
    mz,
    M,
    part,
    cv,
    ob,
    ld,
    pl_sem,
    ysend,
    yS,
    yD,
    pS,
    xsend,
    xD,
    whole,
    bsend,
    brecv,
    yB,
    cB,
    rsend,
    rrecv,
    zsend,
    zrecv,
    gsend,
    grecv,
    asend,
    arecv,
    fsend,
    frecv,
    ready,
):
    blk = lax.axis_index("blk")
    vox = lax.axis_index("vox")
    x, yh, c = blk // 4, (blk // 2) % 2, blk % 2
    z, yl = vox // 2, vox % 2
    y = yh * 2 + yl
    half = src_v.shape[1] // 2
    vc = half // NQ
    scope = jax.named_scope

    up, down = (y + 1) % NY, (y + 3) % NY
    xd = (x // 2) * 2 + 1 - x % 2
    xs = 3 - x
    me = x * 2 + c
    dev_up, dev_down = device(x, up, z, c), device(x, down, z, c)
    dev_xs, dev_xd = device(xs, y, z, c), device(xd, y, z, c)
    dev_c = device(x, y, z, 1 - c)

    def dev_z(d):
        return device(x, y, (z + NZ + d) % NZ, c)

    def signal(sem, to):
        pl.semaphore_signal(sem, inc=1, device_id=to, device_id_type=MESH)

    barrier = pltpu.get_barrier_semaphore()
    near = (dev_up, dev_down, dev_xs, dev_xd, dev_c, dev_z(1), dev_z(-1))
    for to in near:
        signal(barrier, to)

    h_up, h_down = up // 2, down // 2

    parts, turned = [], []
    for q in range(NQ):
        cuts = 2 if q in (0, NQ - 2) else 1
        for i in range(cuts):
            late = q == NQ - 1 or (q == NQ - 2 and i == 1)
            (turned if late else parts).append((q, i * vc // cuts, vc // cuts))
    last = len(parts)

    def columns(h, q, lo, wide):
        return pl.ds(pl.multiple_of(h * half + q * vc + lo, wide), wide)

    pltpu.make_async_copy(probes_hbm, pr_v, pl_sem).start()
    for q in (0, NQ - 2, *range(2, NQ - 2, 2)):
        for h in range(2):
            at = pl.ds(h * half + q * vc, 2 * vc)
            pltpu.make_async_copy(det_hbm.at[:, at], det_v.at[:, at], ld.at[q // 2, 0]).start()
            pltpu.make_async_copy(src_hbm.at[:, at], src_v.at[:, at], ld.at[q // 2, 1]).start()
    with scope("t_barrier"):
        pl.semaphore_wait(barrier, len(near))

    def spread_word(r):
        d = 2**r
        if r:
            pl.semaphore_wait(ready.at[r - 1], 2)
        if r < 3:
            signal(ready.at[r], dev_z(d))
            signal(ready.at[r], dev_z(-d))

    mine = pl.ds(pl.multiple_of(yh * 64, 64), 64)
    own, other = pl.ds(0, 128), pl.ds(128, 128)
    def swap(fields, here, i, sem, n):
        q, lo, wide = parts[n]
        if q % 2 == 0 and lo == 0 and q < NQ - 2:
            wait_for(D.at[q, pl.ds(0, 256)], ld.at[q // 2, i])
        to = (q, mine, pl.ds(lo, wide))
        send(fields.at[:, columns(h_up, q, lo, wide)], here.at[to], ysend.at[i], sem.at[n], dev_up)
        send(fields.at[:, columns(h_down, q, lo, wide)], here.at[to], ysend.at[i], sem.at[n], dev_down)

    for t in range(last):
        swap(det_v, D, 0, yD, t)
        swap(src_v, S, 1, yS, t)
        if t == 0:
            wait_for(pr_v, pl_sem)
            send(
                pr_v.at[:, pl.ds(pl.multiple_of(h_up * half, half), half)],
                pr_in,
                ysend.at[2],
                pS,
                dev_up,
            )
            spread_word(0)
        if t == 2:
            for i, (fields, there, to) in enumerate(((det_v, XD, dev_xd), (src_v, XS, dev_xs))):
                wait_for(D.at[0, pl.ds(0, 256)], ld.at[NQ // 2 - 1, i])
                for h in range(2):
                    at = pl.ds(h * half + turned[0][0] * vc + turned[0][1], there.shape[2])
                    send(fields.at[:, at], there.at[h], bsend.at[i], brecv.at[i], to)

    theirs = pl.ds(pl.multiple_of(128 + yh * 64, 64), 64)

    def swap_b():
        start = 0
        for n, (q, lo, wide) in enumerate(turned):
            for i, (fields, x_in, here) in enumerate(((det_v, XD, D), (src_v, XS, S))):
                at, x_at = pl.ds(lo, wide), pl.ds(start, wide)
                for h, to in ((h_up, dev_up), (h_down, dev_down)):
                    send(fields.at[:, columns(h, q, lo, wide)], here.at[q, mine, at], ysend.at[i], yB.at[i, n], to)
                if n == 0:
                    wait_for(x_in, brecv.at[i])
                for h, to in ((h_up, dev_up), (h_down, dev_down)):
                    send(x_in.at[h, :, x_at], here.at[q, theirs, at], bsend.at[2 + i], yB.at[i, n], to)
            start += wide

    def pass_b(n):
        q, at = turned[n][0], pl.ds(*turned[n][1:])
        wait_for(D.at[q, pl.ds(0, 256), at], yB.at[0, n])
        send(D.at[q, pl.ds(0, 256), at], D.at[q, pl.ds(256, 256), at], xsend.at[2], cB.at[n], dev_c)

    def pass_own(n):
        q, at = parts[n][0], pl.ds(*parts[n][1:])
        wait_for(D.at[q, own, at], yD.at[n])
        send(D.at[q, own, at], D.at[q, other, at], xsend.at[1], xD.at[n], dev_xd)
        send(D.at[q, own, at], D.at[q, pl.ds(256, 128), at], xsend.at[3], whole.at[n], dev_c)
        wait_for(S.at[q, own, at], yS.at[n])
        send(S.at[q, own, at], S.at[q, other, at], xsend.at[0], whole.at[n], dev_xs)

    def pass_other(n):
        q, at = parts[n][0], pl.ds(*parts[n][1:])
        wait_for(D.at[q, other, at], xD.at[n])
        send(D.at[q, other, at], D.at[q, pl.ds(384, 128), at], xsend.at[4], whole.at[n], dev_c)

    def measure(n):
        q, lo, wide = (parts + turned)[n]
        at = pl.ds(lo, wide)
        if n < last:
            wait_for(D.at[q, pl.ds(0, 384), at], whole.at[n])
        else:
            wait_for(D.at[q, pl.ds(256, 256), at], cB.at[n - last])
            wait_for(S.at[q, :, at], yB.at[1, n - last])
        fields = S[q, :, at].astype(F32)
        p = pr_in[:, q * vc + lo : q * vc + lo + wide].astype(F32)
        det = D[q, :, at]
        for k in range(2):
            weighted = (fields * p[k : k + 1]).astype(BF16)
            sums = lax.dot_general(weighted, det, (((1,), (1,)), ((), ())), preferred_element_type=F32)
            for g in range(4):
                piece = sums[:, g * 128 : (g + 1) * 128].reshape(4, 2, 32, 128)
                for h in range(2):
                    if n:
                        acc[k, 2 * g + h] += piece[:, h]
                    else:
                        acc[k, 2 * g + h] = piece[:, h]

    steps = []
    for t in range(last):
        steps.append((pass_own, t))
        if t == 3:
            steps.append((spread_word, 1))
        if t == 6:
            steps.append((spread_word, 2))
        if t >= 3:
            steps.append((pass_other, t - 3))
        if t >= 5:
            steps.append((measure, t - 5))
    n = last
    steps += [(pass_other, n - 3), (pass_b, 0), (measure, n - 5), (measure, n - 4), (pass_other, n - 2)]
    steps += [(measure, n - 3), (measure, n), (pass_other, n - 1), (pass_b, 1)]
    steps += [(measure, n - 2), (measure, n - 1), (measure, n + 1)]
    for t, (step, n) in enumerate(steps):
        if step is measure and n == 0:
            wait_for(pr_in, pS)
        with scope("g%02d_%s%d" % (t, step.__name__, n)):
            step(n)
        if step is pass_own and n == 3:
            swap_b()

    pairs = NZ // 2
    zp, zb = z // 2, z % 2
    s = 1 - 2 * zb
    away = (4, 3 * s, -3 * s, 2 * s, -2 * s, s, -s, 0)
    groups = [(zp + pairs + o) % pairs for o in away]
    turns = [(k, i) for k in range(2) for i in range(pairs)]
    for k, i in turns:
        for d in (2, 1, 3):
            to = (y + d) % NY
            tx[k, i, to] = acc[k, groups[i], to].astype(BF16)
            send(tx.at[k, i, to], rx.at[k, i, y], rsend, rrecv.at[k, i], device(x, to, z, c))
    spread_word(3)

    for k, i in turns:
        g = groups[i]
        with scope("r%d%d_y" % (k, i)):
            wait_for(rx.at[k, i, pl.ds(0, 3)], rrecv.at[k, i])
        total = acc[k, g, y]
        for d in (1, 2, 3):
            total += rx[k, i, (y + d) % NY].astype(F32)
        zs[k, i] = total.astype(BF16).reshape(2, 16, 128)
        for b in (0, 1) if i < pairs - 1 else (1 - zb,):
            send(zs.at[k, i, b], zr.at[k, z], zsend, zrecv.at[k], device(x, y, g * 2 + b, c))
    for k in range(2):
        zr[k, z] = zs[k, pairs - 1, zb]

    def back_along_z(k):
        with scope("r%d_z" % k):
            wait_for(zr.at[k, pl.ds(0, NZ - 1)], zrecv.at[k])
        total = zr[k, 0].astype(F32)
        for j in range(1, NZ):
            total += zr[k, j].astype(F32)
        mz[k] = total.astype(BF16)
        M[k, zp, y, zb] = mz[k]
        for step in range(NZ // 2, 0, -1):
            for to in (step, -step)[: 1 if step == NZ // 2 else 2]:
                send(mz.at[k], M.at[k, zp, y, zb], gsend, grecv.at[k, zp], dev_z(to))

    block, side = zp // 2, 2 * (zp % 2) - 1
    blocks = [(block + o) % 4 for o in (0, 4 + side, 4 - side, 2)]

    back = groups[::-1]

    def back_along_y(k):
        for i, g in enumerate(back):
            with scope("b%d%d_z" % (k, i)):
                wait_for(zr.at[k, pl.ds(0, 2 if i else 1)], grecv.at[k, g])
            off = (g // 2 - block + 4) % 4
            far = jnp.where((off == 0) | (off == (4 + side) % 4), 0, 1)
            for d in (2, 1, 3):
                send(M.at[k, g, y], M.at[k, g, y], asend, arecv.at[k, far], device(x, (y + d) % NY, z, c))

    def arrived(k, far):
        wait_for(M.at[k, pl.ds(0, 4), pl.ds(0, 3)], arecv.at[k, far])

    def contribution(k, q, lo):
        two = blocks[lo : lo + 2]
        lhs = jnp.concatenate([M[k, pl.ds(2 * g, 2)].reshape(256, 128) for g in two], axis=1)
        det = jnp.concatenate([D[q, pl.ds(pl.multiple_of(g * 128, 128), 128)] for g in two], axis=0)
        bp = jnp.dot(lhs, det, preferred_element_type=F32).reshape(2, 4, 32, vc)
        fields = S[q].astype(F32).reshape(4, 2, 32, vc)
        row = jnp.zeros((8, vc), F32)
        for h in range(2):
            row += jnp.sum((fields[:, h] * bp[h]).reshape(16, 8, vc), axis=0)
        return row

    def front(k):
        with scope("m%d_front" % k):
            arrived(k, 0)
            for q in range(NQ):
                part[k, q] = contribution(k, q, 0)

    def rest(k):
        with scope("m%d_y" % k):
            arrived(k, 1)
        per = NQ // NB
        with scope("m%d_rest" % k):
            for n in range(NB):
                rows = []
                for q in range(n * per, (n + 1) * per):
                    row = jnp.sum(part[k, q] + contribution(k, q, 2), axis=0, keepdims=True)
                    rows += [row[:, i * 128 : (i + 1) * 128] for i in range(vc // 128)]
                cv[k, n] = jnp.concatenate(rows, axis=0)
                for d in (2, 1, 3, 0):
                    for core in range(NC):
                        for to in (up, down):
                            at = device((x + d) % NX, to, z, core)
                            send(cv.at[k, n], ob.at[k, yh, me, n], fsend, frecv.at[k], at)

    def finish(k):
        with scope("f%d_recv" % k):
            wait_for(ob.at[k], frecv.at[k])
        wide = half // NB
        for h in range(2):
            for n in range(NB):
                total = ob[k, h, 0, n]
                for e in range(1, NX * NC):
                    total += ob[k, h, e, n]
                total = total * scale
                for i in range(wide // 128):
                    at = h * half + n * wide + i * 128
                    out[k : k + 1, at : at + 128] = total[i : i + 1]

    back_along_z(0)
    back_along_z(1)
    back_along_y(0)
    back_along_y(1)
    front(0)
    rest(0)
    front(1)
    rest(1)
    finish(0)

    wait_for(det_v, ysend.at[0])
    wait_for(src_v, ysend.at[1])
    wait_for(pr_in, ysend.at[2])
    passed = det_v.at[:, pl.ds(0, 2 * sum(wide for _, _, wide in parts))]
    for i in (0, 1, 3, 4):
        wait_for(passed, xsend.at[i])
    wait_for(det_v.at[:, pl.ds(0, 4 * sum(wide for _, _, wide in turned))], xsend.at[2])
    for i in range(4):
        wait_for(XD, bsend.at[i])
    wait_for(tx.at[:, :, pl.ds(0, 3)], rsend)
    wait_for(zr.at[:, pl.ds(0, NZ - 1)], zsend)
    wait_for(zr.at[:, pl.ds(0, NZ - 1)], gsend)
    wait_for(M.at[:, :, pl.ds(0, 3)], asend)
    wait_for(ob, fsend)
    finish(1)


def shards(src_fields, det_fields, probes):
    rows, voxels = src_fields.shape
    half = voxels // 2
    vc = half // NQ
    sources, detectors = rows * lax.axis_size("blk"), det_fields.shape[0] * lax.axis_size("blk")
    scale = 1.0 / (sources * detectors)
    hbm = pl.BlockSpec(memory_space=pl.ANY)
    given = [pltpu.with_memory_space_constraint(a, pltpu.HBM) for a in (src_fields, det_fields, probes)]
    return pl.pallas_call(
        functools.partial(kernel, scale),
        out_shape=jax.ShapeDtypeStruct((2, voxels), F32),
        in_specs=[hbm] * 3,
        out_specs=pl.BlockSpec(memory_space=pltpu.VMEM),
        scratch_shapes=[
            pltpu.VMEM((64, voxels), BF16),
            pltpu.VMEM((64, voxels), BF16),
            pltpu.VMEM((2, voxels), BF16),
            pltpu.VMEM((2, half), BF16),
            pltpu.VMEM((NQ, 256, vc), BF16),
            pltpu.VMEM((NQ, 512, vc), BF16),
            pltpu.VMEM((2, 64, 3 * vc // 2), BF16),
            pltpu.VMEM((2, 64, 3 * vc // 2), BF16),
            pltpu.VMEM((2, 8, 4, 32, 128), F32),
            pltpu.VMEM((2, 8, 4, 32, 128), BF16),
            pltpu.VMEM((2, 8, 4, 32, 128), BF16),
            pltpu.VMEM((2, 8, 2, 16, 128), BF16),
            pltpu.VMEM((2, NZ, 16, 128), BF16),
            pltpu.VMEM((2, 16, 128), BF16),
            pltpu.VMEM((2, 8, 4, 2, 16, 128), BF16),
            pltpu.VMEM((2, NQ, 8, vc), F32),
            pltpu.VMEM((2, NB, half // NB // 128, 128), F32),
            pltpu.VMEM((2, 2, NX * NC, NB, half // NB // 128, 128), F32),
            DMA((NQ // 2, 2)),
            DMA,
            DMA((3,)),
            DMA((NQ,)),
            DMA((NQ,)),
            DMA,
            DMA((5,)),
            DMA((NQ,)),
            DMA((NQ,)),
            DMA((4,)),
            DMA((2,)),
            DMA((2, 2)),
            DMA((2,)),
            DMA,
            DMA((2, 8)),
            DMA,
            DMA((2,)),
            DMA,
            DMA((2, 8)),
            DMA,
            DMA((2, 2)),
            DMA,
            DMA((2,)),
            pltpu.SemaphoreType.REGULAR((3,)),
        ],
        compiler_params=pltpu.CompilerParams(
            collective_id=0, has_side_effects=True, vmem_limit_bytes=50_000_000
        ),
        name="gauss_newton",
    )(*given)


def solution(mesh):
    return jax.shard_map(
        shards,
        mesh=mesh,
        in_specs=(P("blk", "vox"), P("blk", "vox"), P(None, "vox")),
        out_specs=P(None, "vox"),
        check_vma=False,
    )
```

```python
import functools

import jax
import jax.numpy as jnp
from jax import lax
from jax.experimental import pallas as pl
from jax.experimental.pallas import tpu as pltpu
from jax.sharding import PartitionSpec as P

MESH = pl.DeviceIdType.MESH
BF16 = jnp.bfloat16
F32 = jnp.float32
DMA = pltpu.SemaphoreType.DMA

NX, NY, NZ, NC = 4, 4, 16, 2
NQ = 8
NB = 2


def device(x, y, z, c):
    return (x * 4 + (y // 2) * 2 + c, z * 2 + y % 2)


def send(src, dst, send_sem, recv_sem, to):
    pltpu.make_async_remote_copy(
        src_ref=src, dst_ref=dst, send_sem=send_sem, recv_sem=recv_sem, device_id=to, device_id_type=MESH
    ).start()


def wait_for(ref, sem):
    pltpu.make_async_copy(ref, ref, sem).wait()


def kernel(
    scale,
    src_hbm,
    det_hbm,
    probes_hbm,
    out,
    src_v,
    det_v,
    pr_v,
    pr_in,
    S,
    D,
    XS,
    XD,
    acc,
    tx,
    rx,
    zs,
    zr,
    mz,
    M,
    part,
    cv,
    ob,
    ld,
    pl_sem,
    ysend,
    yS,
    yD,
    pS,
    xsend,
    xD,
    whole,
    bsend,
    brecv,
    yB,
    cB,
    rsend,
    rrecv,
    zsend,
    zrecv,
    gsend,
    grecv,
    asend,
    arecv,
    fsend,
    frecv,
    ready,
):
    blk = lax.axis_index("blk")
    vox = lax.axis_index("vox")
    x, yh, c = blk // 4, (blk // 2) % 2, blk % 2
    z, yl = vox // 2, vox % 2
    y = yh * 2 + yl
    half = src_v.shape[1] // 2
    vc = half // NQ
    scope = jax.named_scope

    up, down = (y + 1) % NY, (y + 3) % NY
    xd = (x // 2) * 2 + 1 - x % 2
    xs = 3 - x
    me = x * 2 + c
    dev_up, dev_down = device(x, up, z, c), device(x, down, z, c)
    dev_xs, dev_xd = device(xs, y, z, c), device(xd, y, z, c)
    dev_c = device(x, y, z, 1 - c)

    def dev_z(d):
        return device(x, y, (z + NZ + d) % NZ, c)

    def signal(sem, to):
        pl.semaphore_signal(sem, inc=1, device_id=to, device_id_type=MESH)

    barrier = pltpu.get_barrier_semaphore()
    near = (dev_up, dev_down, dev_xs, dev_xd, dev_c, dev_z(1), dev_z(-1))
    for to in near:
        signal(barrier, to)

    h_up, h_down = up // 2, down // 2

    parts, turned = [], []
    for q in range(NQ):
        cuts = 2 if q in (0, NQ - 2) else 1
        for i in range(cuts):
            late = q == NQ - 1 or (q == NQ - 2 and i == 1)
            (turned if late else parts).append((q, i * vc // cuts, vc // cuts))
    last = len(parts)

    def columns(h, q, lo, wide):
        return pl.ds(pl.multiple_of(h * half + q * vc + lo, wide), wide)

    pltpu.make_async_copy(probes_hbm, pr_v, pl_sem).start()
    for q in (0, NQ - 2, *range(2, NQ - 2, 2)):
        for h in range(2):
            at = pl.ds(h * half + q * vc, 2 * vc)
            pltpu.make_async_copy(det_hbm.at[:, at], det_v.at[:, at], ld.at[q // 2, 0]).start()
            pltpu.make_async_copy(src_hbm.at[:, at], src_v.at[:, at], ld.at[q // 2, 1]).start()
    with scope("t_barrier"):
        pl.semaphore_wait(barrier, len(near))

    def spread_word(r):
        d = 2**r
        if r:
            pl.semaphore_wait(ready.at[r - 1], 2)
        if r < 3:
            signal(ready.at[r], dev_z(d))
            signal(ready.at[r], dev_z(-d))

    mine = pl.ds(pl.multiple_of(yh * 64, 64), 64)
    own, other = pl.ds(0, 128), pl.ds(128, 128)
    def swap(fields, here, i, sem, n):
        q, lo, wide = parts[n]
        if q % 2 == 0 and lo == 0 and q < NQ - 2:
            wait_for(D.at[q, pl.ds(0, 256)], ld.at[q // 2, i])
        to = (q, mine, pl.ds(lo, wide))
        send(fields.at[:, columns(h_up, q, lo, wide)], here.at[to], ysend.at[i], sem.at[n], dev_up)
        send(fields.at[:, columns(h_down, q, lo, wide)], here.at[to], ysend.at[i], sem.at[n], dev_down)

    for t in range(last):
        swap(det_v, D, 0, yD, t)
        swap(src_v, S, 1, yS, t)
        if t == 0:
            wait_for(pr_v, pl_sem)
            send(
                pr_v.at[:, pl.ds(pl.multiple_of(h_up * half, half), half)],
                pr_in,
                ysend.at[2],
                pS,
                dev_up,
            )
            spread_word(0)
        if t == 2:
            for i, (fields, there, to) in enumerate(((det_v, XD, dev_xd), (src_v, XS, dev_xs))):
                wait_for(D.at[0, pl.ds(0, 256)], ld.at[NQ // 2 - 1, i])
                for h in range(2):
                    at = pl.ds(h * half + turned[0][0] * vc + turned[0][1], there.shape[2])
                    send(fields.at[:, at], there.at[h], bsend.at[i], brecv.at[i], to)

    theirs = pl.ds(pl.multiple_of(128 + yh * 64, 64), 64)

    def swap_b():
        start = 0
        for n, (q, lo, wide) in enumerate(turned):
            for i, (fields, x_in, here) in enumerate(((det_v, XD, D), (src_v, XS, S))):
                at, x_at = pl.ds(lo, wide), pl.ds(start, wide)
                for h, to in ((h_up, dev_up), (h_down, dev_down)):
                    send(fields.at[:, columns(h, q, lo, wide)], here.at[q, mine, at], ysend.at[i], yB.at[i, n], to)
                if n == 0:
                    wait_for(x_in, brecv.at[i])
                for h, to in ((h_up, dev_up), (h_down, dev_down)):
                    send(x_in.at[h, :, x_at], here.at[q, theirs, at], bsend.at[2 + i], yB.at[i, n], to)
            start += wide

    def pass_b(n):
        q, at = turned[n][0], pl.ds(*turned[n][1:])
        wait_for(D.at[q, pl.ds(0, 256), at], yB.at[0, n])
        send(D.at[q, pl.ds(0, 256), at], D.at[q, pl.ds(256, 256), at], xsend.at[2], cB.at[n], dev_c)

    def pass_own(n):
        q, at = parts[n][0], pl.ds(*parts[n][1:])
        wait_for(D.at[q, own, at], yD.at[n])
        send(D.at[q, own, at], D.at[q, other, at], xsend.at[1], xD.at[n], dev_xd)
        send(D.at[q, own, at], D.at[q, pl.ds(256, 128), at], xsend.at[3], whole.at[n], dev_c)
        wait_for(S.at[q, own, at], yS.at[n])
        send(S.at[q, own, at], S.at[q, other, at], xsend.at[0], whole.at[n], dev_xs)

    def pass_other(n):
        q, at = parts[n][0], pl.ds(*parts[n][1:])
        wait_for(D.at[q, other, at], xD.at[n])
        send(D.at[q, other, at], D.at[q, pl.ds(384, 128), at], xsend.at[4], whole.at[n], dev_c)

    def measure(n):
        q, lo, wide = (parts + turned)[n]
        at = pl.ds(lo, wide)
        if n < last:
            wait_for(D.at[q, pl.ds(0, 384), at], whole.at[n])
        else:
            wait_for(D.at[q, pl.ds(256, 256), at], cB.at[n - last])
            wait_for(S.at[q, :, at], yB.at[1, n - last])
        fields = S[q, :, at].astype(F32)
        p = pr_in[:, q * vc + lo : q * vc + lo + wide].astype(F32)
        det = D[q, :, at]
        for k in range(2):
            weighted = (fields * p[k : k + 1]).astype(BF16)
            sums = lax.dot_general(weighted, det, (((1,), (1,)), ((), ())), preferred_element_type=F32)
            for g in range(4):
                piece = sums[:, g * 128 : (g + 1) * 128].reshape(4, 2, 32, 128)
                for h in range(2):
                    if n:
                        acc[k, 2 * g + h] += piece[:, h]
                    else:
                        acc[k, 2 * g + h] = piece[:, h]

    steps = []
    for t in range(last):
        steps.append((pass_own, t))
        if t == 3:
            steps.append((spread_word, 1))
        if t == 6:
            steps.append((spread_word, 2))
        if t >= 3:
            steps.append((pass_other, t - 3))
        if t >= 5:
            steps.append((measure, t - 5))
    n = last
    steps += [(pass_other, n - 3), (pass_b, 0), (measure, n - 5), (measure, n - 4), (pass_other, n - 2)]
    steps += [(measure, n - 3), (measure, n), (pass_other, n - 1), (pass_b, 1)]
    steps += [(measure, n - 2), (measure, n - 1), (measure, n + 1)]
    for t, (step, n) in enumerate(steps):
        if step is measure and n == 0:
            wait_for(pr_in, pS)
        with scope("g%02d_%s%d" % (t, step.__name__, n)):
            step(n)
        if step is pass_own and n == 3:
            swap_b()

    pairs = NZ // 2
    zp, zb = z // 2, z % 2
    s = 1 - 2 * zb
    away = (4, 3 * s, -3 * s, 2 * s, -2 * s, s, -s, 0)
    groups = [(zp + pairs + o) % pairs for o in away]
    turns = [(k, i) for k in range(2) for i in range(pairs)]
    for k, i in turns:
        for d in (2, 1, 3):
            to = (y + d) % NY
            tx[k, i, to] = acc[k, groups[i], to].astype(BF16)
            send(tx.at[k, i, to], rx.at[k, i, y], rsend, rrecv.at[k, i], device(x, to, z, c))
    spread_word(3)

    for k, i in turns:
        g = groups[i]
        with scope("r%d%d_y" % (k, i)):
            wait_for(rx.at[k, i, pl.ds(0, 3)], rrecv.at[k, i])
        total = acc[k, g, y]
        for d in (1, 2, 3):
            total += rx[k, i, (y + d) % NY].astype(F32)
        zs[k, i] = total.astype(BF16).reshape(2, 16, 128)
        for b in (0, 1) if i < pairs - 1 else (1 - zb,):
            send(zs.at[k, i, b], zr.at[k, z], zsend, zrecv.at[k], device(x, y, g * 2 + b, c))
    for k in range(2):
        zr[k, z] = zs[k, pairs - 1, zb]

    def back_along_z(k):
        with scope("r%d_z" % k):
            wait_for(zr.at[k, pl.ds(0, NZ - 1)], zrecv.at[k])
        total = zr[k, 0].astype(F32)
        for j in range(1, NZ):
            total += zr[k, j].astype(F32)
        mz[k] = total.astype(BF16)
        M[k, zp, y, zb] = mz[k]
        for step in range(NZ // 2, 0, -1) if k else range(1, NZ // 2 + 1):
            for to in (step, -step)[: 1 if step == NZ // 2 else 2]:
                send(mz.at[k], M.at[k, zp, y, zb], gsend, grecv.at[k, zp], dev_z(to))

    block, side = zp // 2, 2 * (zp % 2) - 1
    blocks = [(block + o) % 4 for o in (0, 4 + side, 4 - side, 2)]

    back = groups[::-1]

    def back_along_y(k):
        for i, g in enumerate(back):
            with scope("b%d%d_z" % (k, i)):
                wait_for(zr.at[k, pl.ds(0, 2 if i else 1)], grecv.at[k, g])
            off = (g // 2 - block + 4) % 4
            far = jnp.where((off == 0) | (off == (4 + side) % 4), 0, 1)
            for d in (2, 1, 3):
                send(M.at[k, g, y], M.at[k, g, y], asend, arecv.at[k, far], device(x, (y + d) % NY, z, c))

    def arrived(k, far):
        wait_for(M.at[k, pl.ds(0, 4), pl.ds(0, 3)], arecv.at[k, far])

    def contribution(k, q, lo):
        two = blocks[lo : lo + 2]
        lhs = jnp.concatenate([M[k, pl.ds(2 * g, 2)].reshape(256, 128) for g in two], axis=1)
        det = jnp.concatenate([D[q, pl.ds(pl.multiple_of(g * 128, 128), 128)] for g in two], axis=0)
        bp = jnp.dot(lhs, det, preferred_element_type=F32).reshape(2, 4, 32, vc)
        fields = S[q].astype(F32).reshape(4, 2, 32, vc)
        row = jnp.zeros((8, vc), F32)
        for h in range(2):
            row += jnp.sum((fields[:, h] * bp[h]).reshape(16, 8, vc), axis=0)
        return row

    def front(k):
        with scope("m%d_front" % k):
            arrived(k, 0)
            for q in range(NQ):
                part[k, q] = contribution(k, q, 0)

    def rest(k):
        with scope("m%d_y" % k):
            arrived(k, 1)
        per = NQ // NB
        with scope("m%d_rest" % k):
            for n in range(NB):
                rows = []
                for q in range(n * per, (n + 1) * per):
                    row = jnp.sum(part[k, q] + contribution(k, q, 2), axis=0, keepdims=True)
                    rows += [row[:, i * 128 : (i + 1) * 128] for i in range(vc // 128)]
                cv[k, n] = jnp.concatenate(rows, axis=0)
                for d in (2, 1, 3, 0):
                    for core in range(NC):
                        for to in (up, down):
                            at = device((x + d) % NX, to, z, core)
                            send(cv.at[k, n], ob.at[k, yh, me, n], fsend, frecv.at[k], at)

    def finish(k):
        with scope("f%d_recv" % k):
            wait_for(ob.at[k], frecv.at[k])
        wide = half // NB
        for h in range(2):
            for n in range(NB):
                total = ob[k, h, 0, n]
                for e in range(1, NX * NC):
                    total += ob[k, h, e, n]
                total = total * scale
                for i in range(wide // 128):
                    at = h * half + n * wide + i * 128
                    out[k : k + 1, at : at + 128] = total[i : i + 1]

    back_along_z(0)
    back_along_z(1)
    back_along_y(0)
    back_along_y(1)
    front(0)
    rest(0)
    front(1)
    rest(1)
    finish(0)

    wait_for(det_v, ysend.at[0])
    wait_for(src_v, ysend.at[1])
    wait_for(pr_in, ysend.at[2])
    passed = det_v.at[:, pl.ds(0, 2 * sum(wide for _, _, wide in parts))]
    for i in (0, 1, 3, 4):
        wait_for(passed, xsend.at[i])
    wait_for(det_v.at[:, pl.ds(0, 4 * sum(wide for _, _, wide in turned))], xsend.at[2])
    for i in range(4):
        wait_for(XD, bsend.at[i])
    wait_for(tx.at[:, :, pl.ds(0, 3)], rsend)
    wait_for(zr.at[:, pl.ds(0, NZ - 1)], zsend)
    wait_for(zr.at[:, pl.ds(0, NZ - 1)], gsend)
    wait_for(M.at[:, :, pl.ds(0, 3)], asend)
    wait_for(ob, fsend)
    finish(1)


def shards(src_fields, det_fields, probes):
    rows, voxels = src_fields.shape
    half = voxels // 2
    vc = half // NQ
    sources, detectors = rows * lax.axis_size("blk"), det_fields.shape[0] * lax.axis_size("blk")
    scale = 1.0 / (sources * detectors)
    hbm = pl.BlockSpec(memory_space=pl.ANY)
    given = [pltpu.with_memory_space_constraint(a, pltpu.HBM) for a in (src_fields, det_fields, probes)]
    return pl.pallas_call(
        functools.partial(kernel, scale),
        out_shape=jax.ShapeDtypeStruct((2, voxels), F32),
        in_specs=[hbm] * 3,
        out_specs=pl.BlockSpec(memory_space=pltpu.VMEM),
        scratch_shapes=[
            pltpu.VMEM((64, voxels), BF16),
            pltpu.VMEM((64, voxels), BF16),
            pltpu.VMEM((2, voxels), BF16),
            pltpu.VMEM((2, half), BF16),
            pltpu.VMEM((NQ, 256, vc), BF16),
            pltpu.VMEM((NQ, 512, vc), BF16),
            pltpu.VMEM((2, 64, 3 * vc // 2), BF16),
            pltpu.VMEM((2, 64, 3 * vc // 2), BF16),
            pltpu.VMEM((2, 8, 4, 32, 128), F32),
            pltpu.VMEM((2, 8, 4, 32, 128), BF16),
            pltpu.VMEM((2, 8, 4, 32, 128), BF16),
            pltpu.VMEM((2, 8, 2, 16, 128), BF16),
            pltpu.VMEM((2, NZ, 16, 128), BF16),
            pltpu.VMEM((2, 16, 128), BF16),
            pltpu.VMEM((2, 8, 4, 2, 16, 128), BF16),
            pltpu.VMEM((2, NQ, 8, vc), F32),
            pltpu.VMEM((2, NB, half // NB // 128, 128), F32),
            pltpu.VMEM((2, 2, NX * NC, NB, half // NB // 128, 128), F32),
            DMA((NQ // 2, 2)),
            DMA,
            DMA((3,)),
            DMA((NQ,)),
            DMA((NQ,)),
            DMA,
            DMA((5,)),
            DMA((NQ,)),
            DMA((NQ,)),
            DMA((4,)),
            DMA((2,)),
            DMA((2, 2)),
            DMA((2,)),
            DMA,
            DMA((2, 8)),
            DMA,
            DMA((2,)),
            DMA,
            DMA((2, 8)),
            DMA,
            DMA((2, 2)),
            DMA,
            DMA((2,)),
            pltpu.SemaphoreType.REGULAR((3,)),
        ],
        compiler_params=pltpu.CompilerParams(
            collective_id=0, has_side_effects=True, vmem_limit_bytes=50_000_000
        ),
        name="gauss_newton",
    )(*given)


def solution(mesh):
    return jax.shard_map(
        shards,
        mesh=mesh,
        in_specs=(P("blk", "vox"), P("blk", "vox"), P(None, "vox")),
        out_specs=P(None, "vox"),
        check_vma=False,
    )
```
